64 devices in a mesh: req: 4 (over x, y), cp: 16 (over z, core).
Axes of the slice: x: 2, y: 2, z: 8, core: 2. Of those that a mesh axis runs over, the one named last changes fastest.
The devices are a block of a 4x4x8 slice.
Arguments:
- hidden: bfloat16 [8192, 2048], P(('req', 'cp')), parts along dimension 0
- positions: int32 [8192], P(('req', 'cp')), parts along dimension 0
- segments: int32 [8192], P(('req', 'cp')), parts along dimension 0
- gain_1: bfloat16 [3, 2048], replicated
- gain_2: bfloat16 [3, 2048], replicated
- w_q: bfloat16 [3, 2048, 32, 64], replicated
- w_k: bfloat16 [3, 2048, 8, 64], replicated
- w_v: bfloat16 [3, 2048, 8, 64], replicated
- w_o: bfloat16 [3, 32, 64, 2048], replicated
- w_1: bfloat16 [3, 2048, 8192], replicated
- w_3: bfloat16 [3, 2048, 8192], replicated
- w_2: bfloat16 [3, 8192, 2048], replicated
Outputs:
- output 1: bfloat16 [8192, 2048], P(('req', 'cp')), parts along dimension 0
- output 2: bfloat16 [3, 8192, 512], P(None, 'req', 'cp'), parts along dimension 1
- output 3: bfloat16 [3, 8192, 512], P(None, 'req', 'cp'), parts along dimension 1
There are 4 independent parts. The reference program is written for one: setup_inputs(seed, part) draws one part's arguments, and reference() takes and returns one part's arrays. A program takes and returns all parts, laid end to end along the dimension named above; an argument that names none is the same for every part.
All inputs are finite; a program needn't handle non-finite values.
Results may differ from the reference program's by a relative error of at most 0.02.
Values are sent between devices in bfloat16 or wider.
A program may use at most 768 MiB of HBM per device.

```python
import jax
import jax.numpy as jnp
from jax import lax

D_MODEL = 2048
Q_HEADS = 32
KV_HEADS = 8
HEAD_DIM = 64
FF_DIM = 8192
LAYERS = 3
TOKENS_DEV = 128
CP_SIZE = 16
REQUESTS = 4
ROPE_THETA = 10000

SEQ_LEN = TOKENS_DEV * CP_SIZE
HALF_LEN = TOKENS_DEV // 2
Q_GROUP = Q_HEADS // KV_HEADS
Q_WIDTH = Q_HEADS * HEAD_DIM
KV_WIDTH = KV_HEADS * HEAD_DIM
NORM_EPS = 1e-5
QK_GAIN = 1.4
MASK_FILL = -1e30


def storage_natural():
    row_ids = jnp.arange(SEQ_LEN, dtype=jnp.int32)
    owner_dev = row_ids // TOKENS_DEV
    within = row_ids % TOKENS_DEV
    block_idx = jnp.where(within < HALF_LEN, owner_dev, 2 * CP_SIZE - 1 - owner_dev)
    return block_idx * HALF_LEN + within % HALF_LEN


def normal_weight(key_w, shape, fan_in, w_gain):
    return (jax.random.normal(key_w, shape, jnp.float32) * (w_gain * fan_in ** -0.5)).astype(jnp.bfloat16)


def setup_inputs(seed: int = 0, part: int = 0) -> dict:
    part_key = jax.random.fold_in(jax.random.key(seed), part)
    key_x, key_cut = jax.random.split(part_key, 2)
    w_keys = jax.random.split(jax.random.key(seed + 1), 9)
    natural = storage_natural()
    cut_points = jnp.sort(jax.random.permutation(key_cut, SEQ_LEN - 1)[: REQUESTS - 1] + 1).astype(jnp.int32)
    segments = jnp.sum((natural[:, None] >= cut_points[None, :]).astype(jnp.int32), axis=1).astype(jnp.int32)
    seg_starts = jnp.concatenate([jnp.zeros((1,), jnp.int32), cut_points])
    positions = (natural - seg_starts[segments]).astype(jnp.int32)
    hidden = jax.random.normal(key_x, (SEQ_LEN, D_MODEL), jnp.float32).astype(jnp.bfloat16)
    gain_1 = jax.random.uniform(w_keys[0], (LAYERS, D_MODEL), jnp.float32, 0.5, 1.5).astype(jnp.bfloat16)
    gain_2 = jax.random.uniform(w_keys[1], (LAYERS, D_MODEL), jnp.float32, 0.5, 1.5).astype(jnp.bfloat16)
    return dict(
        hidden=hidden,
        positions=positions,
        segments=segments,
        gain_1=gain_1,
        gain_2=gain_2,
        w_q=normal_weight(w_keys[2], (LAYERS, D_MODEL, Q_HEADS, HEAD_DIM), D_MODEL, QK_GAIN),
        w_k=normal_weight(w_keys[3], (LAYERS, D_MODEL, KV_HEADS, HEAD_DIM), D_MODEL, QK_GAIN),
        w_v=normal_weight(w_keys[4], (LAYERS, D_MODEL, KV_HEADS, HEAD_DIM), D_MODEL, 1.0),
        w_o=normal_weight(w_keys[5], (LAYERS, Q_HEADS, HEAD_DIM, D_MODEL), Q_WIDTH, 1.0),
        w_1=normal_weight(w_keys[6], (LAYERS, D_MODEL, FF_DIM), D_MODEL, 1.0),
        w_3=normal_weight(w_keys[7], (LAYERS, D_MODEL, FF_DIM), D_MODEL, 1.0),
        w_2=normal_weight(w_keys[8], (LAYERS, FF_DIM, D_MODEL), FF_DIM, 1.0),
    )


def rms_norm(residual, gain_row):
    resid_f32 = residual.astype(jnp.float32)
    inv_rms = lax.rsqrt(jnp.mean(resid_f32 * resid_f32, axis=-1, keepdims=True) + NORM_EPS)
    return (resid_f32 * inv_rms * gain_row.astype(jnp.float32)).astype(jnp.bfloat16)


def apply_rope(proj, cos_t, sin_t):
    half_dim = proj.shape[-1] // 2
    front_half = proj[..., :half_dim]
    back_half = proj[..., half_dim:]
    cos_b = cos_t[..., None, :]
    sin_b = sin_t[..., None, :]
    return jnp.concatenate([front_half * cos_b - back_half * sin_b, back_half * cos_b + front_half * sin_b], axis=-1)


def mlp_block(residual, gain_row, w_up1, w_up3, w_down):
    normed = rms_norm(residual, gain_row)
    gate_pre = jnp.dot(normed, w_up1, preferred_element_type=jnp.float32)
    up_pre = jnp.dot(normed, w_up3, preferred_element_type=jnp.float32)
    gated_act = (jax.nn.silu(gate_pre) * up_pre).astype(jnp.bfloat16)
    return (residual.astype(jnp.float32) + jnp.dot(gated_act, w_down, preferred_element_type=jnp.float32)).astype(jnp.bfloat16)


def to_natural(cache_rows):
    blocks = cache_rows.reshape(LAYERS, CP_SIZE, 2, HALF_LEN, KV_WIDTH)
    front_part = blocks[:, :, 0]
    back_part = jnp.flip(blocks[:, :, 1], axis=1)
    return jnp.concatenate([front_part, back_part], axis=1).reshape(LAYERS, SEQ_LEN, KV_WIDTH)


def reference(hidden, positions, segments, gain_1, gain_2, w_q, w_k, w_v, w_o, w_1, w_3, w_2):
    inv_freq = ROPE_THETA ** (-2.0 * jnp.arange(HEAD_DIM // 2, dtype=jnp.float32) / HEAD_DIM)
    rot_angle = positions.astype(jnp.float32)[:, None] * inv_freq[None, :]
    cos_t = jnp.cos(rot_angle)
    sin_t = jnp.sin(rot_angle)
    score_scale = HEAD_DIM ** -0.5
    pos_blocks = positions.reshape(CP_SIZE, TOKENS_DEV)
    seg_blocks = segments.reshape(CP_SIZE, TOKENS_DEV)

    def attention(q_rot, k_rot, v_new):
        k_f32 = k_rot.astype(jnp.float32)
        v_f32 = v_new.astype(jnp.float32)
        q_blocks = q_rot.reshape(CP_SIZE, TOKENS_DEV, KV_HEADS, Q_GROUP, HEAD_DIM)

        def one_block(block_in):
            q_blk, pos_blk, seg_blk = block_in
            scores = jnp.einsum('tkgd,skd->kgts', q_blk.astype(jnp.float32), k_f32) * score_scale
            allowed = (seg_blk[:, None] == segments[None, :]) & (positions[None, :] <= pos_blk[:, None])
            scores = jnp.where(allowed, scores, MASK_FILL)
            row_max = jnp.max(scores, axis=-1, keepdims=True)
            exp_scores = jnp.exp(scores - row_max)
            attn_prob = (exp_scores / jnp.sum(exp_scores, axis=-1, keepdims=True)).astype(jnp.bfloat16)
            attn_out = jnp.einsum('kgts,skd->tkgd', attn_prob.astype(jnp.float32), v_f32)
            return attn_out.astype(jnp.bfloat16).reshape(TOKENS_DEV, Q_WIDTH)

        return lax.map(one_block, (q_blocks, pos_blocks, seg_blocks)).reshape(SEQ_LEN, Q_WIDTH)

    def layer_step(residual, params):
        g_one, g_two, wq_l, wk_l, wv_l, wo_l, w1_l, w3_l, w2_l = params
        normed = rms_norm(residual, g_one)
        q_pre = jnp.dot(normed, wq_l.reshape(D_MODEL, Q_WIDTH), preferred_element_type=jnp.float32)
        q_rot = apply_rope(q_pre.reshape(SEQ_LEN, Q_HEADS, HEAD_DIM), cos_t, sin_t).astype(jnp.bfloat16)
        k_pre = jnp.dot(normed, wk_l.reshape(D_MODEL, KV_WIDTH), preferred_element_type=jnp.float32)
        k_rot = apply_rope(k_pre.reshape(SEQ_LEN, KV_HEADS, HEAD_DIM), cos_t, sin_t).astype(jnp.bfloat16)
        v_new = jnp.dot(normed, wv_l.reshape(D_MODEL, KV_WIDTH), preferred_element_type=jnp.float32).astype(jnp.bfloat16)
        attn_out = attention(q_rot, k_rot, v_new.reshape(SEQ_LEN, KV_HEADS, HEAD_DIM))
        residual = (residual.astype(jnp.float32) + jnp.dot(attn_out, wo_l.reshape(Q_WIDTH, D_MODEL), preferred_element_type=jnp.float32)).astype(jnp.bfloat16)
        residual = mlp_block(residual, g_two, w1_l, w3_l, w2_l)
        return residual, (k_rot.reshape(SEQ_LEN, KV_WIDTH), v_new)

    final_hidden, caches = lax.scan(layer_step, hidden, (gain_1, gain_2, w_q, w_k, w_v, w_o, w_1, w_3, w_2))
    return final_hidden, to_natural(caches[0]), to_natural(caches[1])
```

```python
import functools
import math

import jax
import jax.numpy as jnp
from jax import lax
from jax.experimental import pallas as pl
from jax.experimental.pallas import tpu as pltpu
from jax.sharding import PartitionSpec as P

NORM_EPS = 1e-5
ROPE_THETA = 10000.0
MASK_FILL = -1e30
BIG = 3e38
LOG2E = math.log2(math.e)
MESH = pl.DeviceIdType.MESH
F32 = jnp.float32
BF16 = jnp.bfloat16
NT = (((1,), (1,)), ((), ()))
NA = 8
UP, DN, D2D = 0, 1, 2


def kernel(cfg, x_in, pos_in, cos_in, sin_in, g1_in, g2_in, wq, wk, wv, wo, w1, w3, w2,
           x_out, kc, vc,
           ring_a, ring_b, kv, knat, qx, oacc, m_st, l_st, cap, xs, hs, ub, acc,
           sem_a, sem_b, send_sem, recv_sem, cred, csem):
    n_layers, n_cp, nb = cfg["layers"], cfg["n_cp"], cfg["nb"]
    n_tok, d_model = xs.shape
    n_chip = n_cp // 2
    n_kv = oacc.shape[0]
    head_dim = oacc.shape[1]
    lanes = oacc.shape[2]
    q_group = lanes // n_tok
    kvw = n_kv * head_dim
    half = head_dim // 2
    rows_a = ring_a.shape[1]
    cols_b = ring_b.shape[2]
    n_ff = w1.shape[2] // cols_b
    n_q = wq.shape[1] // rows_a
    n_o = wo.shape[1] // rows_a
    n_pos = 2 + n_q + n_o + n_ff
    first_q, first_o, first_w2 = 2, 2 + n_q, 2 + n_q + n_o

    me = lax.axis_index("cp")
    z, c = me // 2, me % 2
    up = ((z + 1) % n_chip) * 2 + c
    dn = ((z + n_chip - 1) % n_chip) * 2 + c
    partner = z * 2 + (1 - c)

    def a_copy(l, pos):
        slot = lax.rem(l * n_pos + pos, NA)
        if isinstance(pos, int):
            if pos == 0:
                src = wk.at[l]
            elif pos == 1:
                src = wv.at[l]
            elif pos < first_o:
                src = wq.at[l, pl.ds((pos - first_q) * rows_a, rows_a), :]
            elif pos < first_w2:
                src = wo.at[l, pl.ds((pos - first_o) * rows_a, rows_a), :]
            else:
                src = w2.at[l, pl.ds((pos - first_w2) * rows_a, rows_a), :]
        else:
            src = w2.at[l, pl.ds(pl.multiple_of((pos - first_w2) * rows_a, rows_a), rows_a), :]
        return pltpu.make_async_copy(src, ring_a.at[slot], sem_a.at[slot])

    def a_slot(l, pos):
        return lax.rem(l * n_pos + pos, NA)

    def b_copy(l, j, t):
        w = w1 if t == 0 else w3
        slot = lax.rem((l * n_ff + j) * 2 + t, nb)
        src = w.at[l, :, pl.ds(pl.multiple_of(j * cols_b, cols_b), cols_b)]
        return pltpu.make_async_copy(src, ring_b.at[slot], sem_b.at[slot])

    def ring_copy(dirn, tile, part):
        ref = kv.at[tile, pl.ds(part * kvw, kvw), :]
        dev = (up, dn, partner)[dirn]
        return pltpu.make_async_remote_copy(
            src_ref=ref, dst_ref=ref, send_sem=send_sem.at[dirn, tile, part],
            recv_sem=recv_sem.at[tile, part], device_id={"cp": dev}, device_id_type=MESH)

    for pos in range(NA):
        a_copy(0, pos).start()
    for j in range(nb // 2):
        for t in range(2):
            b_copy(0, j, t).start()

    barrier = pltpu.get_barrier_semaphore()
    for dev in (up, dn, partner):
        pl.semaphore_signal(barrier, inc=1, device_id={"cp": dev}, device_id_type=MESH)

    xs[...] = x_in[...]
    qx[...] = jnp.zeros_like(qx)
    pl.semaphore_wait(barrier, 3)

    half_tok = n_tok // 2

    def norm_rows(gain):
        blk = 16

        def one(r, carry):
            rows = pl.ds(pl.multiple_of(r * blk, blk), blk)
            v = xs[rows, :].astype(F32)
            inv = lax.rsqrt(jnp.mean(v * v, axis=-1, keepdims=True) + NORM_EPS)
            hs[rows, :] = (v * inv * gain).astype(BF16)
            return carry

        lax.fori_loop(0, n_tok // blk, one, 0, unroll=2)

    def resid_rows():
        blk = 16

        def one(r, carry):
            rows = pl.ds(pl.multiple_of(r * blk, blk), blk)
            xs[rows, :] = (xs[rows, :].astype(F32) + acc[rows, :]).astype(BF16)
            return carry

        lax.fori_loop(0, n_tok // blk, one, 0, unroll=2)

    def rope_t(t):
        nh = t.shape[0] // head_dim
        cos_b = cos_in[...]
        sin_b = sin_in[...]
        outs = []
        for n in range(nh):
            a = t[n * head_dim:n * head_dim + half]
            b = t[n * head_dim + half:(n + 1) * head_dim]
            outs.append(a * cos_b - b * sin_b)
            outs.append(b * cos_b + a * sin_b)
        return outs

    lane = lax.broadcasted_iota(jnp.int32, (1, n_tok), 1)
    n_blk = 2 * n_cp

    def nat_of(tile, idx):
        return jnp.where(idx < half_tok, tile * half_tok + idx, (n_blk - 1 - tile) * half_tok + idx - half_tok)

    def attend(chip):
        nat_q = nat_of(me, lane)
        start_q = nat_q - pos_in[...]
        for s in range(2):
            key = lax.broadcasted_iota(jnp.int32, (n_tok, n_tok), 0)
            nat_k = nat_of(chip * 2 + s, key)
            ok = (nat_k >= start_q) & (nat_k <= nat_q)
            cap[s * n_tok:(s + 1) * n_tok, :] = jnp.where(ok, BIG, MASK_FILL)
            for p in range(n_kv // 2):
                kt = kv[chip * 2 + s, p * 2 * head_dim:(p + 1) * 2 * head_dim, :]
                knat[p, s * n_tok:(s + 1) * n_tok, :] = kt.T

        def one_g(i, carry):
            for gg in range(4):
                g = i * 4 + gg
                k_blk = knat[i * 2 + gg // 2]
                rows = pl.ds(pl.multiple_of(kvw + g * head_dim, head_dim), head_dim)
                v_blk = jnp.concatenate([kv[chip * 2, rows, :], kv[chip * 2 + 1, rows, :]], axis=1)
                m_row = m_st[g]
                l_row = l_st[g]
                for hf in range(q_group // 2):
                    ls = slice(hf * 2 * n_tok, (hf + 1) * 2 * n_tok)
                    s_t = jnp.dot(k_blk, qx[g, :, ls], preferred_element_type=F32)
                    cap2 = jnp.concatenate([cap[...], cap[...]], axis=1)
                    s_t = jnp.minimum(s_t, cap2) * LOG2E
                    m_old = m_row[0:1, ls]
                    m_new = jnp.maximum(m_old, jnp.max(s_t, axis=0, keepdims=True))
                    e = jnp.exp2(s_t - m_new)
                    alpha = jnp.exp2(m_old - m_new)
                    m_st[g, 0:1, ls] = m_new
                    l_st[g, 0:1, ls] = l_row[0:1, ls] * alpha + jnp.sum(e, axis=0, keepdims=True)
                    pv = jnp.dot(v_blk, e.astype(BF16), preferred_element_type=F32)
                    oacc[g, :, ls] = oacc[g, :, ls] * alpha + pv
            return carry

        lax.fori_loop(0, n_kv // 4, one_g, 0)

    def tile_of(dist):
        return lax.rem(z + dist + n_chip, n_chip) * 2 + c

    far = n_chip // 2

    def layer(l, carry):
        has_next = l + 1 < n_layers

        norm_rows(g1_in[l])

        @pl.when(l > 0)
        def _():
            for i in range(3):
                pl.semaphore_wait(cred.at[i], 1)

        for part in range(2):
            a_copy(l, part).wait()
            t = lax.dot_general(ring_a[a_slot(l, part)], hs[...], NT, preferred_element_type=F32)
            if part == 0:
                for n, blk in enumerate(rope_t(t)):
                    kv[me, n * half:(n + 1) * half, :] = blk.astype(BF16)
            else:
                kv[me, kvw:2 * kvw, :] = t.astype(BF16)
            for dirn in (UP, DN, D2D):
                ring_copy(dirn, me, part).start()
            a_copy(l, part + NA).start()

        for i in range(n_q):
            pos = first_q + i
            a_copy(l, pos).wait()
            t = lax.dot_general(ring_a[a_slot(l, pos)], hs[...], NT, preferred_element_type=F32)
            for n, blk in enumerate(rope_t(t)):
                head = i * (rows_a // head_dim) + n // 2
                g, slot = head // q_group, head % q_group
                r0 = (g % 2) * head_dim + (n % 2) * half
                qx[g, r0:r0 + half, slot * n_tok:(slot + 1) * n_tok] = (blk.astype(BF16).astype(F32) * head_dim ** -0.5).astype(BF16)
            a_copy(l, pos + NA).start()

        m_st[...] = jnp.full_like(m_st, MASK_FILL * LOG2E)
        l_st[...] = jnp.zeros_like(l_st)
        oacc[...] = jnp.zeros_like(oacc)

        def step(k, carry):
            dist = (k + 1) // 2

            def serve(part):
                lo, hi = tile_of(-dist), tile_of(dist)

                @pl.when(dist < far)
                def _():
                    ring_copy(UP, lo, part).wait_recv()

                    @pl.when((dist < far - 1) | (part == 0))
                    def _():
                        ring_copy(UP, lo, part).start()

                    ring_copy(D2D, lo, part).start()
                    ring_copy(DN, hi, part).wait_recv()

                    @pl.when((dist < far - 1) | (part == 1))
                    def _():
                        ring_copy(DN, hi, part).start()

                    ring_copy(D2D, hi, part).start()

                @pl.when(dist == far)
                def _():
                    ring_copy(UP, lo, part).wait_recv()
                    ring_copy(D2D, lo, part).start()

            @pl.when(k % 2 == 1)
            def _():
                serve(0)
                serve(1)

            chip = jnp.where(k % 2 == 1, z - dist + n_chip, z + dist) % n_chip
            other = chip * 2 + 1 - c
            for part in range(2):
                ring_copy(D2D, other, part).wait_recv()
            attend(chip)
            return carry

        lax.fori_loop(0, n_chip, step, 0)

        r0 = pl.multiple_of(me * (kvw // n_cp), kvw // n_cp)
        ck = pltpu.make_async_copy(kv.at[:, pl.ds(r0, kvw // n_cp), :], kc.at[l], csem.at[0])
        cv = pltpu.make_async_copy(kv.at[:, pl.ds(kvw + r0, kvw // n_cp), :], vc.at[l], csem.at[1])
        ck.start()
        cv.start()

        for i in range(n_o):
            pos = first_o + i
            a_copy(l, pos).wait()
            n_g = rows_a // (q_group * head_dim)
            parts = []
            for gg in range(n_g):
                g = i * n_g + gg
                o = oacc[g] * (1.0 / l_st[g, 0:1, :])
                for hh in range(q_group):
                    parts.append(o[:, hh * n_tok:(hh + 1) * n_tok])
            o_t = jnp.concatenate(parts, axis=0)
            o_n = o_t.T.astype(BF16)
            y = jnp.dot(o_n, ring_a[a_slot(l, pos)], preferred_element_type=F32)
            if i == 0:
                acc[...] = y
            else:
                acc[...] += y
            a_copy(l, pos + NA).start()
        resid_rows()

        ck.wait()
        cv.wait()
        for part in range(2):
            for dirn in (UP, DN, D2D):
                ring_copy(dirn, me, part).wait_send()
            for dist in range(1, far):
                lo, hi = tile_of(-dist), tile_of(dist)
                if dist < far - 1 or part == 0:
                    ring_copy(UP, lo, part).wait_send()
                if dist < far - 1 or part == 1:
                    ring_copy(DN, hi, part).wait_send()
                ring_copy(D2D, lo, part).wait_send()
                ring_copy(D2D, hi, part).wait_send()
            ring_copy(D2D, tile_of(far), part).wait_send()

        @pl.when(has_next)
        def _():
            pl.semaphore_signal(cred.at[DN], inc=1, device_id={"cp": up}, device_id_type=MESH)
            pl.semaphore_signal(cred.at[UP], inc=1, device_id={"cp": dn}, device_id_type=MESH)
            pl.semaphore_signal(cred.at[D2D], inc=1, device_id={"cp": partner}, device_id_type=MESH)

        norm_rows(g2_in[l])

        def up_part(j):
            for t in range(2):
                b_copy(l, j, t).wait()
            s0 = lax.rem((l * n_ff + j) * 2, nb)
            a = jnp.dot(hs[...], ring_b[s0], preferred_element_type=F32)
            b = jnp.dot(hs[...], ring_b[s0 + 1], preferred_element_type=F32)
            ub[lax.rem(j, 2)] = (jax.nn.silu(a) * b).astype(BF16)

        def up_refill(j):
            j2 = j + nb // 2
            l2 = l + j2 // n_ff

            @pl.when(l2 < n_layers)
            def _():
                for t in range(2):
                    b_copy(l2, lax.rem(j2, n_ff), t).start()

        def down_refill(j):
            @pl.when(j + NA < n_ff)
            def _():
                a_copy(l, first_w2 + j + NA).start()

            for pos in range(NA):
                @pl.when((j + NA - n_ff == pos) & has_next)
                def _():
                    a_copy(l + 1, pos).start()

        def mlp(j, carry):
            a_copy(l, first_w2 + j - 1).wait()
            up_part(j)
            acc[...] += jnp.dot(ub[lax.rem(j - 1, 2)], ring_a[a_slot(l, first_w2 + j - 1)], preferred_element_type=F32)
            up_refill(j)
            down_refill(j - 1)
            return carry

        acc[...] = jnp.zeros_like(acc)
        up_part(0)
        up_refill(0)
        lax.fori_loop(1, n_ff, mlp, 0)
        a_copy(l, first_w2 + n_ff - 1).wait()
        acc[...] += jnp.dot(ub[(n_ff - 1) % 2], ring_a[a_slot(l, first_w2 + n_ff - 1)], preferred_element_type=F32)
        down_refill(n_ff - 1)
        resid_rows()
        return carry

    lax.fori_loop(0, n_layers, layer, 0)
    x_out[...] = xs[...]


def to_natural(cache):
    n_layers, n_dev, n_cols, n_tok = cache.shape
    blocks = cache.reshape(n_layers, n_dev, n_cols, 2, n_tok // 2)
    front = blocks[:, :, :, 0]
    back = jnp.flip(blocks[:, :, :, 1], axis=1)
    both = jnp.concatenate([front, back], axis=1)
    both = jnp.transpose(both, (0, 2, 1, 3)).reshape(n_layers, n_cols, n_dev * n_tok)
    return jnp.transpose(both, (0, 2, 1))


def solution(mesh):
    n_cp = mesh.shape["cp"]
    row_spec = P(("req", "cp"), None)
    tok_spec = P(("req", "cp"))
    rep_spec = P()
    cache_spec = P(None, "req", "cp")

    def local_step(hidden, positions, segments, gain_1, gain_2, w_q, w_k, w_v, w_o, w_1, w_3, w_2):
        n_layers, d_model, n_heads, head_dim = w_q.shape
        n_kv = w_k.shape[2]
        n_tok = hidden.shape[0]
        kvw = n_kv * head_dim
        q_group = n_heads // n_kv
        rows_a, cols_b, nb = kvw, 512, 16
        inv_freq = ROPE_THETA ** (-2.0 * jnp.arange(head_dim // 2, dtype=F32) / head_dim)
        angle = inv_freq[:, None] * positions.astype(F32)[None, :]
        cos_t, sin_t = jnp.cos(angle), jnp.sin(angle)

        def turned(w):
            return jnp.transpose(w, (0, 2, 3, 1)).reshape(n_layers, -1, d_model)

        cfg = dict(layers=n_layers, n_cp=n_cp, nb=nb)
        vmem = pl.BlockSpec(memory_space=pltpu.VMEM)
        hbm = pl.BlockSpec(memory_space=pl.ANY)
        cache = jax.ShapeDtypeStruct((n_layers, n_cp, kvw // n_cp, n_tok), BF16)
        x, k_c, v_c = pl.pallas_call(
            functools.partial(kernel, cfg),
            out_shape=(jax.ShapeDtypeStruct(hidden.shape, BF16), cache, cache),
            in_specs=[vmem] * 6 + [hbm] * 7,
            out_specs=(vmem, hbm, hbm),
            scratch_shapes=[
                pltpu.VMEM((NA, rows_a, d_model), BF16),
                pltpu.VMEM((nb, d_model, cols_b), BF16),
                pltpu.VMEM((n_cp, 2 * kvw, n_tok), BF16),
                pltpu.VMEM((n_kv // 2, 2 * n_tok, 2 * head_dim), BF16),
                pltpu.VMEM((n_kv, 2 * head_dim, q_group * n_tok), BF16),
                pltpu.VMEM((n_kv, head_dim, q_group * n_tok), F32),
                pltpu.VMEM((n_kv, 8, q_group * n_tok), F32),
                pltpu.VMEM((n_kv, 8, q_group * n_tok), F32),
                pltpu.VMEM((2 * n_tok, n_tok), F32),
                pltpu.VMEM((n_tok, d_model), BF16),
                pltpu.VMEM((n_tok, d_model), BF16),
                pltpu.VMEM((2, n_tok, cols_b), BF16),
                pltpu.VMEM((n_tok, d_model), F32),
                pltpu.SemaphoreType.DMA((NA,)),
                pltpu.SemaphoreType.DMA((nb,)),
                pltpu.SemaphoreType.DMA((3, n_cp, 2)),
                pltpu.SemaphoreType.DMA((n_cp, 2)),
                pltpu.SemaphoreType.REGULAR((3,)),
                pltpu.SemaphoreType.DMA((2,)),
            ],
            compiler_params=pltpu.CompilerParams(
                collective_id=0, has_side_effects=True, vmem_limit_bytes=67043328),
            name="prefill",
        )(
            hidden, positions[None, :], cos_t, sin_t,
            gain_1.astype(F32)[:, None, :], gain_2.astype(F32)[:, None, :],
            turned(w_q), turned(w_k), turned(w_v), w_o.reshape(n_layers, -1, d_model), w_1, w_3, w_2,
        )
        return x, to_natural(k_c), to_natural(v_c)

    return jax.shard_map(
        local_step,
        mesh=mesh,
        in_specs=(row_spec, tok_spec, tok_spec) + (rep_spec,) * 9,
        out_specs=(row_spec, cache_spec, cache_spec),
        check_vma=False,
    )
```

```python
import functools
import math

import jax
import jax.numpy as jnp
from jax import lax
from jax.experimental import pallas as pl
from jax.experimental.pallas import tpu as pltpu
from jax.sharding import PartitionSpec as P

NORM_EPS = 1e-5
ROPE_THETA = 10000.0
MASK_FILL = -1e30
BIG = 3e38
LOG2E = math.log2(math.e)
MESH = pl.DeviceIdType.MESH
F32 = jnp.float32
BF16 = jnp.bfloat16
NT = (((1,), (1,)), ((), ()))
NA = 4
NB = 16
AHEAD = 2
UP, DN, D2D = 0, 1, 2


def kernel(cfg, x_in, pos_in, cos_in, sin_in, g1_in, g2_in, wq, wk, wv, wo, w1, w3, w2,
           x_out, kc, vc,
           ring_a, ring_b, kv, kvt, knat, qx, oacc, m_st, l_st, cap, cbuf, xs, h2, ub, acc, psend, precv, gains,
           sem_a, sem_b, send_sem, recv_sem, hs_sem, hr_sem, ps_sem, pr_sem, cred, csem):
    n_layers, n_cp, nb = cfg["layers"], cfg["n_cp"], cfg["nb"]
    n_tok, d_model = xs.shape
    half_tok = n_tok // 2
    n_chip = n_cp // 2
    n_kv, head_dim, lanes = oacc.shape
    q_group = lanes // n_tok
    lane_f = lanes // 2
    kvw = n_kv * head_dim
    half = head_dim // 2
    rows_a = ring_a.shape[1]
    k_b, cols_b = ring_b.shape[1:]
    own_ff = ub.shape[1]
    n_up = own_ff // cols_b
    n_dn = d_model // cols_b
    n_kh = own_ff // k_b
    n_pair = n_up + n_dn
    ahead_b = nb // 2
    n_q = wq.shape[1] // rows_a
    n_o = wo.shape[1] // rows_a
    n_pos = 2 + n_q + n_o
    first_q, first_o = 2, 2 + n_q
    n_col = kvw // n_cp

    me = lax.axis_index("cp")
    z, c = me // 2, me % 2
    up = ((z + 1) % n_chip) * 2 + c
    dn = ((z + n_chip - 1) % n_chip) * 2 + c
    partner = z * 2 + (1 - c)

    def a_slot(l, pos):
        return lax.rem(l * n_pos + pos, NA)

    def a_copy(l, pos):
        if pos >= n_pos:
            l, pos = l + 1, pos - n_pos
        slot = a_slot(l, pos)
        if pos == 0:
            src = wk.at[l]
        elif pos == 1:
            src = wv.at[l]
        elif pos < first_o:
            src = wq.at[l, pl.ds((pos - first_q) * rows_a, rows_a), :]
        else:
            src = wo.at[l, pl.ds((pos - first_o) * rows_a, rows_a), :]
        return pltpu.make_async_copy(src, ring_a.at[slot], sem_a.at[slot])

    def a_refill(l, pos):
        if pos + NA < n_pos:
            a_copy(l, pos + NA).start()
        else:
            @pl.when(l + 1 < n_layers)
            def _():
                a_copy(l, pos + NA).start()

    def b_slot(l, q, t):
        return lax.rem((l * n_pair + q) * 2 + t, nb)

    def up_copy(l, j, t):
        slot = b_slot(l, j, t)
        col = pl.multiple_of(c * own_ff + j * cols_b, cols_b)
        return pltpu.make_async_copy((w1, w3)[t].at[l, :, pl.ds(col, cols_b)], ring_b.at[slot], sem_b.at[slot])

    def dn_copy(l, n, t):
        slot = b_slot(l, n_up + n, t)
        row = pl.multiple_of(c * own_ff + t * k_b, k_b)
        col = pl.multiple_of(n * cols_b, cols_b)
        return pltpu.make_async_copy(w2.at[l, pl.ds(row, k_b), pl.ds(col, cols_b)], ring_b.at[slot], sem_b.at[slot])

    def b_refill(l, q):
        q2 = q + ahead_b
        l2 = l + q2 // n_pair
        q3 = lax.rem(q2, n_pair)

        @pl.when((l2 < n_layers) & (q3 < n_up))
        def _():
            for t in range(2):
                up_copy(l2, q3, t).start()

        @pl.when((l2 < n_layers) & (q3 >= n_up))
        def _():
            for t in range(2):
                dn_copy(l2, q3 - n_up, t).start()

    def ring_copy(dirn, tile, part):
        ref = kv.at[tile, pl.ds(part * kvw, kvw), :]
        dev = (up, dn, partner)[dirn]
        return pltpu.make_async_remote_copy(
            src_ref=ref, dst_ref=ref, send_sem=send_sem.at[dirn, tile, part],
            recv_sem=recv_sem.at[tile, part], device_id={"cp": dev}, device_id_type=MESH)

    def h_copy(i):
        rows = pl.ds(i * half_tok, half_tok)
        return pltpu.make_async_remote_copy(
            src_ref=h2.at[0, rows, :], dst_ref=h2.at[1, rows, :], send_sem=hs_sem.at[i],
            recv_sem=hr_sem.at[i], device_id={"cp": partner}, device_id_type=MESH)

    def p_copy(n):
        return pltpu.make_async_remote_copy(
            src_ref=psend.at[n], dst_ref=precv.at[n], send_sem=ps_sem.at[n],
            recv_sem=pr_sem.at[n], device_id={"cp": partner}, device_id_type=MESH)

    for pos in range(NA):
        a_copy(0, pos).start()
    for q in range(ahead_b):
        for t in range(2):
            (up_copy(0, q, t) if q < n_up else dn_copy(0, q - n_up, t)).start()

    barrier = pltpu.get_barrier_semaphore()
    for dev in (up, dn, partner):
        pl.semaphore_signal(barrier, inc=1, device_id={"cp": dev}, device_id_type=MESH)

    xs[...] = x_in[...]
    qx[...] = jnp.zeros_like(qx)
    for i in range(n_layers):
        gains[0, i, 0:1, :] = g1_in[i:i + 1, :].astype(F32)
        gains[1, i, 0:1, :] = g2_in[i:i + 1, :].astype(F32)
    pl.semaphore_wait(barrier, 3)

    blk = 16

    def norm_rows(gain, first, count):
        def one(r, carry):
            rows = pl.ds(pl.multiple_of(first + r * blk, blk), blk)
            v = xs[rows, :].astype(F32)
            inv = lax.rsqrt(jnp.mean(v * v, axis=-1, keepdims=True) + NORM_EPS)
            h2[0, rows, :] = (v * inv * gain).astype(BF16)
            return carry

        lax.fori_loop(0, count // blk, one, 0, unroll=2)

    def rope_t(t):
        cos_b = cos_in[...]
        sin_b = sin_in[...]
        outs = []
        for n in range(t.shape[0] // head_dim):
            a = t[n * head_dim:n * head_dim + half]
            b = t[n * head_dim + half:(n + 1) * head_dim]
            outs.append(a * cos_b - b * sin_b)
            outs.append(b * cos_b + a * sin_b)
        return outs

    def fronts(parts):
        return jnp.concatenate([p[:, :half_tok] for p in parts], axis=1)

    def backs(parts):
        return jnp.concatenate([p[:, half_tok:] for p in parts], axis=1)

    n_unit = 2 * n_chip
    lane = lax.rem(lax.broadcasted_iota(jnp.int32, (1, n_tok), 1), half_tok)
    nat_qs = (me * half_tok + lane, (2 * n_cp - 1 - me) * half_tok + lane)

    def retile(chip):
        step_r = 256
        for r in range(0, 2 * kvw, step_r):
            t0 = kv[chip * 2, r:r + step_r, :]
            t1 = kv[chip * 2 + 1, r:r + step_r, :]
            kvt[r:r + step_r, :n_tok] = fronts([t0, t1])
            kvt[r:r + step_r, n_tok:] = backs([t1, t0])

    def cache_cols(chip):
        r0 = pl.multiple_of(me * n_col, n_col)
        for t in range(2):
            rows = kvt[pl.ds(t * kvw + r0, n_col), :]
            cbuf[t, :, pl.ds(pl.multiple_of(chip * n_tok, n_tok), n_tok)] = rows[:, :n_tok]
            cbuf[t, :, pl.ds(pl.multiple_of((n_unit - 1 - chip) * n_tok, n_tok), n_tok)] = rows[:, n_tok:]

    def attend(chip, blocks):
        retile(chip)
        cache_cols(chip)
        units = max(u for _, u in blocks)
        for p in range(n_kv // 2):
            rows = slice(p * 2 * head_dim, (p + 1) * 2 * head_dim)
            for u in range(units):
                knat[p, u * n_tok:(u + 1) * n_tok, :] = kvt[rows, u * n_tok:(u + 1) * n_tok].T
        key = lax.broadcasted_iota(jnp.int32, (n_tok, n_tok), 0)
        for qh, n_u in blocks:
            start_q = nat_qs[qh] - pos_in[qh:qh + 1, :]
            for u in range(n_u):
                nat_k = (chip if u == 0 else n_unit - 1 - chip) * n_tok + key
                ok = (nat_k >= start_q) & (nat_k <= nat_qs[qh])
                cap[qh, u * n_tok:(u + 1) * n_tok, :] = jnp.where(ok, BIG, MASK_FILL)

        jobs = [(g, qh, n_u * n_tok) for g in range(n_kv) for qh, n_u in blocks]

        def scores(g, qh, n_k):
            return jnp.dot(knat[g // 2, :n_k, :], qx[g, :, qh * lane_f:(qh + 1) * lane_f], preferred_element_type=F32)

        ahead = [scores(*job) for job in jobs[:AHEAD]]
        for n, (g, qh, n_k) in enumerate(jobs):
            ls = slice(qh * lane_f, (qh + 1) * lane_f)
            capv = cap[qh, :n_k, :]
            capv = jnp.concatenate([capv] * (lane_f // n_tok), axis=1)
            s_t = jnp.minimum(ahead.pop(0), capv) * LOG2E
            if n + AHEAD < len(jobs):
                ahead.append(scores(*jobs[n + AHEAD]))
            m_old = m_st[g, 0:1, ls]
            m_new = jnp.maximum(m_old, jnp.max(s_t, axis=0, keepdims=True))
            e = jnp.exp2(s_t - m_new)
            alpha = jnp.exp2(m_old - m_new)
            m_st[g, 0:1, ls] = m_new
            l_st[g, 0:1, ls] = l_st[g, 0:1, ls] * alpha + jnp.sum(e, axis=0, keepdims=True)
            rows = slice(kvw + g * head_dim, kvw + (g + 1) * head_dim)
            pv = jnp.dot(kvt[rows, :n_k], e.astype(BF16), preferred_element_type=F32)
            oacc[g, :, ls] = oacc[g, :, ls] * alpha + pv

    def tile_of(dist):
        return lax.rem(z + dist + n_chip, n_chip) * 2 + c

    far = n_chip // 2

    def serve(part, dist):
        lo, hi = tile_of(-dist), tile_of(dist)
        if dist < far or part == 0:
            ring_copy(UP, lo, part).wait_recv()
            if dist < far - 1 or (dist == far - 1 and part == 0):
                ring_copy(UP, lo, part).start()
            ring_copy(D2D, lo, part).start()
        if dist < far or part == 1:
            ring_copy(DN, hi, part).wait_recv()
            if dist < far - 1 or (dist == far - 1 and part == 1):
                ring_copy(DN, hi, part).start()
            ring_copy(D2D, hi, part).start()

    plan = {1: [(0, 1), (1, 1)]}
    for d in range(2, far):
        plan[2 * d - 2] = [(0, d)]
        plan[2 * d - 1] = [(1, d)]
    plan[2 * far - 2] = [(0, far), (1, far)]

    def layer(l, carry):
        has_next = l + 1 < n_layers

        norm_rows(gains[0, l, 0:1, :], 0, n_tok)

        @pl.when(l > 0)
        def _():
            for i in range(3):
                pl.semaphore_wait(cred.at[i], 1)

        for part in range(2):
            a_copy(l, part).wait()
            t = lax.dot_general(ring_a[a_slot(l, part)], h2[0], NT, preferred_element_type=F32)
            if part == 0:
                for n, b in enumerate(rope_t(t)):
                    kv[me, n * half:(n + 1) * half, :] = b.astype(BF16)
            else:
                kv[me, kvw:2 * kvw, :] = t.astype(BF16)
            for dirn in (UP, DN, D2D):
                ring_copy(dirn, me, part).start()
            a_refill(l, part)

        for i in range(n_q):
            pos = first_q + i
            a_copy(l, pos).wait()
            t = lax.dot_general(ring_a[a_slot(l, pos)], h2[0], NT, preferred_element_type=F32)
            outs = [(b.astype(BF16).astype(F32) * head_dim ** -0.5).astype(BF16) for b in rope_t(t)]
            n_g = rows_a // (q_group * head_dim)
            for gg in range(n_g):
                g = i * n_g + gg
                for hb in range(2):
                    parts = [outs[2 * (gg * q_group + hh) + hb] for hh in range(q_group)]
                    r0 = (g % 2) * head_dim + hb * half
                    qx[g, r0:r0 + half, :lane_f] = fronts(parts)
                    qx[g, r0:r0 + half, lane_f:] = backs(parts)
            a_refill(l, pos)

        m_st[...] = jnp.full_like(m_st, MASK_FILL * LOG2E)
        l_st[...] = jnp.zeros_like(l_st)
        oacc[...] = jnp.zeros_like(oacc)

        for part in range(2):
            ring_copy(D2D, partner, part).wait_recv()
        attend(z, [(0, 1), (1, 2)])

        def step(k, carry):
            dist = (k + 1) // 2
            for at, todo in plan.items():
                @pl.when(k == at)
                def _():
                    for part, d in todo:
                        serve(part, d)
            chip = jnp.where(k % 2 == 1, z - dist + n_chip, z + dist) % n_chip
            other = chip * 2 + 1 - c
            for part in range(2):
                ring_copy(D2D, other, part).wait_recv()

            @pl.when(chip < z)
            def _():
                attend(chip, [(0, 1), (1, 1)])

            @pl.when(chip > z)
            def _():
                attend(chip, [(1, 2)])

            return carry

        lax.fori_loop(1, n_chip, step, 0)

        ck = pltpu.make_async_copy(cbuf.at[0], kc.at[l], csem.at[0])
        cv = pltpu.make_async_copy(cbuf.at[1], vc.at[l], csem.at[1])
        ck.start()
        cv.start()

        for i in range(n_o):
            pos = first_o + i
            a_copy(l, pos).wait()
            n_g = rows_a // (q_group * head_dim)
            parts = []
            for gg in range(n_g):
                g = i * n_g + gg
                o = oacc[g] * (1.0 / l_st[g, 0:1, :])
                for hh in range(q_group):
                    f0 = hh * half_tok
                    parts.append(jnp.concatenate(
                        [o[:, f0:f0 + half_tok], o[:, lane_f + f0:lane_f + f0 + half_tok]], axis=1))
            o_n = jnp.concatenate(parts, axis=0).T.astype(BF16)
            y = jnp.dot(o_n, ring_a[a_slot(l, pos)], preferred_element_type=F32)
            if i == 0:
                acc[...] = y
            else:
                acc[...] += y
            a_refill(l, pos)

        gain = gains[1, l, 0:1, :]
        for i in range(2):
            def one(r, carry):
                rows = pl.ds(pl.multiple_of(i * half_tok + r * blk, blk), blk)
                xs[rows, :] = (xs[rows, :].astype(F32) + acc[rows, :]).astype(BF16)
                return carry

            lax.fori_loop(0, half_tok // blk, one, 0, unroll=2)
            norm_rows(gain, i * half_tok, half_tok)
            h_copy(i).start()

        ck.wait()
        cv.wait()
        for part in range(2):
            for dirn in (UP, DN, D2D):
                ring_copy(dirn, me, part).wait_send()
            for dist in range(1, far):
                lo, hi = tile_of(-dist), tile_of(dist)
                if dist < far - 1 or part == 0:
                    ring_copy(UP, lo, part).wait_send()
                if dist < far - 1 or part == 1:
                    ring_copy(DN, hi, part).wait_send()
                ring_copy(D2D, lo, part).wait_send()
                ring_copy(D2D, hi, part).wait_send()
            ring_copy(D2D, tile_of(far), part).wait_send()

        @pl.when(has_next)
        def _():
            pl.semaphore_signal(cred.at[DN], inc=1, device_id={"cp": up}, device_id_type=MESH)
            pl.semaphore_signal(cred.at[UP], inc=1, device_id={"cp": dn}, device_id_type=MESH)
            pl.semaphore_signal(cred.at[D2D], inc=1, device_id={"cp": partner}, device_id_type=MESH)

        for i in range(2):
            h_copy(i).wait_recv()

        def up_step(j, carry):
            for t in range(2):
                up_copy(l, j, t).wait()
            h_all = h2[...].reshape(2 * n_tok, d_model)
            a = jnp.dot(h_all, ring_b[b_slot(l, j, 0)], preferred_element_type=F32)
            b = jnp.dot(h_all, ring_b[b_slot(l, j, 1)], preferred_element_type=F32)
            ub[:, pl.ds(pl.multiple_of(j * cols_b, cols_b), cols_b)] = (jax.nn.silu(a) * b).astype(BF16)
            b_refill(l, j)
            return carry

        lax.fori_loop(0, n_up, up_step, 0)

        def dn_step(n, carry):
            for t in range(2):
                dn_copy(l, n, t).wait()
            y = jnp.dot(ub[:, :k_b], ring_b[b_slot(l, n_up + n, 0)], preferred_element_type=F32)
            y += jnp.dot(ub[:, k_b:], ring_b[b_slot(l, n_up + n, 1)], preferred_element_type=F32)
            psend[n] = y[n_tok:]
            p_copy(n).start()
            acc[:, pl.ds(pl.multiple_of(n * cols_b, cols_b), cols_b)] = y[:n_tok]
            b_refill(l, n_up + n)
            return carry

        lax.fori_loop(0, n_dn, dn_step, 0)
        for i in range(2):
            h_copy(i).wait_send()

        def merge(n, carry):
            p_copy(n).wait()
            cols = pl.ds(pl.multiple_of(n * cols_b, cols_b), cols_b)
            xs[:, cols] = (xs[:, cols].astype(F32) + (acc[:, cols] + precv[n])).astype(BF16)
            return carry

        lax.fori_loop(0, n_dn, merge, 0)
        return carry

    lax.fori_loop(0, n_layers, layer, 0)
    x_out[...] = xs[...]


def solution(mesh):
    n_cp = mesh.shape["cp"]
    row_spec = P(("req", "cp"), None)
    tok_spec = P(("req", "cp"))
    rep_spec = P()
    cache_spec = P(None, "req", "cp")

    def local_step(hidden, positions, segments, gain_1, gain_2, w_q, w_k, w_v, w_o, w_1, w_3, w_2):
        n_layers, d_model, n_heads, head_dim = w_q.shape
        n_kv = w_k.shape[2]
        n_tok = hidden.shape[0]
        kvw = n_kv * head_dim
        q_group = n_heads // n_kv
        d_ff = w_1.shape[2]
        rows_a, cols_b, k_b, nb = kvw, d_model // 4, d_ff // 4, NB
        inv_freq = ROPE_THETA ** (-2.0 * jnp.arange(head_dim // 2, dtype=F32) / head_dim)
        angle = inv_freq[:, None] * positions.astype(F32)[None, :]
        cos_t, sin_t = jnp.cos(angle), jnp.sin(angle)
        pos_2 = positions.reshape(2, n_tok // 2)
        pos_2 = jnp.concatenate([pos_2, pos_2], axis=1)

        def turned(w):
            return jnp.transpose(w, (0, 2, 3, 1)).reshape(n_layers, -1, d_model)

        cfg = dict(layers=n_layers, n_cp=n_cp, nb=nb)
        vmem = pl.BlockSpec(memory_space=pltpu.VMEM)
        hbm = pl.BlockSpec(memory_space=pl.ANY)
        n_all = n_cp * n_tok
        cache = jax.ShapeDtypeStruct((n_layers, kvw // n_cp, n_all), BF16)
        x, k_c, v_c = pl.pallas_call(
            functools.partial(kernel, cfg),
            out_shape=(jax.ShapeDtypeStruct(hidden.shape, BF16), cache, cache),
            in_specs=[vmem] * 6 + [hbm] * 7,
            out_specs=(vmem, hbm, hbm),
            scratch_shapes=[
                pltpu.VMEM((NA, rows_a, d_model), BF16),
                pltpu.VMEM((nb, k_b, cols_b), BF16),
                pltpu.VMEM((n_cp, 2 * kvw, n_tok), BF16),
                pltpu.VMEM((2 * kvw, 2 * n_tok), BF16),
                pltpu.VMEM((n_kv // 2, 2 * n_tok, 2 * head_dim), BF16),
                pltpu.VMEM((n_kv, 2 * head_dim, q_group * n_tok), BF16),
                pltpu.VMEM((n_kv, head_dim, q_group * n_tok), F32),
                pltpu.VMEM((n_kv, 8, q_group * n_tok), F32),
                pltpu.VMEM((n_kv, 8, q_group * n_tok), F32),
                pltpu.VMEM((2, 2 * n_tok, n_tok), F32),
                pltpu.VMEM((2, kvw // n_cp, n_all), BF16),
                pltpu.VMEM((n_tok, d_model), BF16),
                pltpu.VMEM((2, n_tok, d_model), BF16),
                pltpu.VMEM((2 * n_tok, d_ff // 2), BF16),
                pltpu.VMEM((n_tok, d_model), F32),
                pltpu.VMEM((d_model // cols_b, n_tok, cols_b), F32),
                pltpu.VMEM((d_model // cols_b, n_tok, cols_b), F32),
                pltpu.VMEM((2, n_layers, 8, d_model), F32),
                pltpu.SemaphoreType.DMA((NA,)),
                pltpu.SemaphoreType.DMA((nb,)),
                pltpu.SemaphoreType.DMA((3, n_cp, 2)),
                pltpu.SemaphoreType.DMA((n_cp, 2)),
                pltpu.SemaphoreType.DMA((2,)),
                pltpu.SemaphoreType.DMA((2,)),
                pltpu.SemaphoreType.DMA((d_model // cols_b,)),
                pltpu.SemaphoreType.DMA((d_model // cols_b,)),
                pltpu.SemaphoreType.REGULAR((3,)),
                pltpu.SemaphoreType.DMA((2,)),
            ],
            compiler_params=pltpu.CompilerParams(
                collective_id=0, has_side_effects=True, vmem_limit_bytes=67043328),
            name="prefill",
        )(
            hidden, pos_2, cos_t, sin_t, gain_1, gain_2,
            turned(w_q), turned(w_k), turned(w_v), w_o.reshape(n_layers, -1, d_model), w_1, w_3, w_2,
        )
        return x, jnp.transpose(k_c, (0, 2, 1)), jnp.transpose(v_c, (0, 2, 1))

    return jax.shard_map(
        local_step,
        mesh=mesh,
        in_specs=(row_spec, tok_spec, tok_spec) + (rep_spec,) * 9,
        out_specs=(row_spec, cache_spec, cache_spec),
        check_vma=False,
    )
```

```python
import functools
import math

import jax
import jax.numpy as jnp
from jax import lax
from jax.experimental import pallas as pl
from jax.experimental.pallas import tpu as pltpu
from jax.sharding import PartitionSpec as P

NORM_EPS = 1e-5
ROPE_THETA = 10000.0
MASK_FILL = -1e30
BIG = 3e38
LOG2E = math.log2(math.e)
MESH = pl.DeviceIdType.MESH
F32 = jnp.float32
BF16 = jnp.bfloat16
NT = (((1,), (1,)), ((), ()))
NA = 4
NB = 16
AHEAD = 2
UP, DN, D2D = 0, 1, 2


def kernel(cfg, x_in, pos_in, cos_in, sin_in, g1_in, g2_in, wq, wk, wv, wo, w1, w3, w2,
           x_out, kc, vc,
           ring_a, ring_b, kv, kvt, knat, qx, oacc, m_st, l_st, cap, cbuf, o_n, xs, h2, ub, acc, psend, precv, gains,
           sem_a, sem_b, send_sem, recv_sem, fs_sem, fr_sem, hs_sem, hr_sem, ps_sem, pr_sem, cred, csem):
    n_layers, n_cp, nb = cfg["layers"], cfg["n_cp"], cfg["nb"]
    n_tok, d_model = xs.shape
    half_tok = n_tok // 2
    n_chip = n_cp // 2
    n_kv, head_dim, lanes = oacc.shape
    q_group = lanes // n_tok
    lane_f = lanes // 2
    kvw = n_kv * head_dim
    half = head_dim // 2
    rows_a = ring_a.shape[1]
    k_b, cols_b = ring_b.shape[1:]
    own_ff = ub.shape[1]
    n_up = own_ff // cols_b
    n_dn = d_model // cols_b
    n_kh = own_ff // k_b
    n_pair = n_up + n_dn
    ahead_b = nb // 2
    n_q = wq.shape[1] // rows_a
    n_o = wo.shape[1] // rows_a
    n_pos = 2 + n_q + n_o
    first_q, first_o = 2, 2 + n_q
    n_col = kvw // n_cp

    me = lax.axis_index("cp")
    z, c = me // 2, me % 2
    up = ((z + 1) % n_chip) * 2 + c
    dn = ((z + n_chip - 1) % n_chip) * 2 + c
    partner = z * 2 + (1 - c)

    def a_slot(l, pos):
        return lax.rem(l * n_pos + pos, NA)

    def a_copy(l, pos):
        if pos >= n_pos:
            l, pos = l + 1, pos - n_pos
        slot = a_slot(l, pos)
        if pos == 0:
            src = wk.at[l]
        elif pos == 1:
            src = wv.at[l]
        elif pos < first_o:
            src = wq.at[l, pl.ds((pos - first_q) * rows_a, rows_a), :]
        else:
            src = wo.at[l, pl.ds((pos - first_o) * rows_a, rows_a), :]
        return pltpu.make_async_copy(src, ring_a.at[slot], sem_a.at[slot])

    def a_refill(l, pos):
        if pos + NA < n_pos:
            a_copy(l, pos + NA).start()
        else:
            @pl.when(l + 1 < n_layers)
            def _():
                a_copy(l, pos + NA).start()

    def b_slot(l, q, t):
        return lax.rem((l * n_pair + q) * 2 + t, nb)

    def up_copy(l, j, t):
        slot = b_slot(l, j, t)
        col = pl.multiple_of(c * own_ff + j * cols_b, cols_b)
        return pltpu.make_async_copy((w1, w3)[t].at[l, :, pl.ds(col, cols_b)], ring_b.at[slot], sem_b.at[slot])

    def dn_copy(l, n, t):
        slot = b_slot(l, n_up + n, t)
        row = pl.multiple_of(c * own_ff + t * k_b, k_b)
        col = pl.multiple_of(n * cols_b, cols_b)
        return pltpu.make_async_copy(w2.at[l, pl.ds(row, k_b), pl.ds(col, cols_b)], ring_b.at[slot], sem_b.at[slot])

    def b_refill(l, q):
        q2 = q + ahead_b
        l2 = l + q2 // n_pair
        q3 = lax.rem(q2, n_pair)

        @pl.when((l2 < n_layers) & (q3 < n_up))
        def _():
            for t in range(2):
                up_copy(l2, q3, t).start()

        @pl.when((l2 < n_layers) & (q3 >= n_up))
        def _():
            for t in range(2):
                dn_copy(l2, q3 - n_up, t).start()

    def ring_copy(dirn, tile, part):
        ref = kv.at[tile, pl.ds(part * kvw, kvw), :]
        dev = (up, dn, partner)[dirn]
        return pltpu.make_async_remote_copy(
            src_ref=ref, dst_ref=ref, send_sem=send_sem.at[dirn, tile, part],
            recv_sem=recv_sem.at[tile, part], device_id={"cp": dev}, device_id_type=MESH)

    def far_copy(dirn, tile, part):
        ref = kv.at[tile, pl.ds(part * kvw + dirn * (kvw // 2), kvw // 2), :]
        return pltpu.make_async_remote_copy(
            src_ref=ref, dst_ref=ref, send_sem=fs_sem.at[dirn, part],
            recv_sem=fr_sem.at[dirn, part], device_id={"cp": (up, dn)[dirn]}, device_id_type=MESH)

    def h_copy(i):
        rows = pl.ds(i * half_tok, half_tok)
        return pltpu.make_async_remote_copy(
            src_ref=h2.at[0, rows, :], dst_ref=h2.at[1, rows, :], send_sem=hs_sem.at[i],
            recv_sem=hr_sem.at[i], device_id={"cp": partner}, device_id_type=MESH)

    def p_copy(n):
        return pltpu.make_async_remote_copy(
            src_ref=psend.at[n], dst_ref=precv.at[n], send_sem=ps_sem.at[n],
            recv_sem=pr_sem.at[n], device_id={"cp": partner}, device_id_type=MESH)

    for pos in range(NA):
        a_copy(0, pos).start()
    barrier = pltpu.get_barrier_semaphore()
    for dev in (up, dn, partner):
        pl.semaphore_signal(barrier, inc=1, device_id={"cp": dev}, device_id_type=MESH)

    xs[...] = x_in[...]
    qx[...] = jnp.zeros_like(qx)
    for i in range(n_layers):
        gains[0, i, 0:1, :] = g1_in[i:i + 1, :].astype(F32)
        gains[1, i, 0:1, :] = g2_in[i:i + 1, :].astype(F32)
    pl.semaphore_wait(barrier, 3)

    blk = 16

    def norm_rows(gain, first, count):
        def one(r, carry):
            rows = pl.ds(pl.multiple_of(first + r * blk, blk), blk)
            v = xs[rows, :].astype(F32)
            inv = lax.rsqrt(jnp.mean(v * v, axis=-1, keepdims=True) + NORM_EPS)
            h2[0, rows, :] = (v * inv * gain).astype(BF16)
            return carry

        lax.fori_loop(0, count // blk, one, 0, unroll=2)

    def rope_t(t):
        cos_b = cos_in[...]
        sin_b = sin_in[...]
        outs = []
        for n in range(t.shape[0] // head_dim):
            a = t[n * head_dim:n * head_dim + half]
            b = t[n * head_dim + half:(n + 1) * head_dim]
            outs.append(a * cos_b - b * sin_b)
            outs.append(b * cos_b + a * sin_b)
        return outs

    def project(ref):
        mid = rows_a // 2
        return [lax.dot_general(ref[i * mid:(i + 1) * mid, :], h2[0], NT, preferred_element_type=F32) for i in range(2)]

    def fronts(parts):
        return jnp.concatenate([p[:, :half_tok] for p in parts], axis=1)

    def backs(parts):
        return jnp.concatenate([p[:, half_tok:] for p in parts], axis=1)

    n_unit = 2 * n_chip
    lane = lax.rem(lax.broadcasted_iota(jnp.int32, (1, n_tok), 1), half_tok)
    nat_qs = (me * half_tok + lane, (2 * n_cp - 1 - me) * half_tok + lane)

    def retile(chip):
        step_r = 256
        for r in range(0, 2 * kvw, step_r):
            t0 = kv[chip * 2, r:r + step_r, :]
            t1 = kv[chip * 2 + 1, r:r + step_r, :]
            kvt[r:r + step_r, :n_tok] = fronts([t0, t1])
            kvt[r:r + step_r, n_tok:] = backs([t1, t0])

    def cache_cols(chip):
        r0 = pl.multiple_of(me * n_col, n_col)
        for t in range(2):
            rows = kvt[pl.ds(t * kvw + r0, n_col), :]
            cbuf[t, :, pl.ds(pl.multiple_of(chip * n_tok, n_tok), n_tok)] = rows[:, :n_tok]
            cbuf[t, :, pl.ds(pl.multiple_of((n_unit - 1 - chip) * n_tok, n_tok), n_tok)] = rows[:, n_tok:]

    def attend(chip, blocks):
        retile(chip)
        cache_cols(chip)
        units = max(u for _, u in blocks)
        for p in range(n_kv // 2):
            rows = slice(p * 2 * head_dim, (p + 1) * 2 * head_dim)
            for u in range(units):
                knat[p, u * n_tok:(u + 1) * n_tok, :] = kvt[rows, u * n_tok:(u + 1) * n_tok].T
        key = lax.broadcasted_iota(jnp.int32, (n_tok, n_tok), 0)
        for qh, n_u in blocks:
            start_q = nat_qs[qh] - pos_in[qh:qh + 1, :]
            for u in range(n_u):
                nat_k = (chip if u == 0 else n_unit - 1 - chip) * n_tok + key
                ok = (nat_k >= start_q) & (nat_k <= nat_qs[qh])
                cap[qh, u * n_tok:(u + 1) * n_tok, :] = jnp.where(ok, BIG, MASK_FILL)

        jobs = [(g, qh, n_u * n_tok) for g in range(n_kv) for qh, n_u in blocks]

        def scores(g, qh, n_k):
            return jnp.dot(knat[g // 2, :n_k, :], qx[g, :, qh * lane_f:(qh + 1) * lane_f], preferred_element_type=F32)

        ahead = [scores(*job) for job in jobs[:AHEAD]]
        for n, (g, qh, n_k) in enumerate(jobs):
            ls = slice(qh * lane_f, (qh + 1) * lane_f)
            capv = cap[qh, :n_k, :]
            capv = jnp.concatenate([capv] * (lane_f // n_tok), axis=1)
            s_t = jnp.minimum(ahead.pop(0), capv) * LOG2E
            if n + AHEAD < len(jobs):
                ahead.append(scores(*jobs[n + AHEAD]))
            m_old = m_st[g, 0:1, ls]
            m_new = jnp.maximum(m_old, jnp.max(s_t, axis=0, keepdims=True))
            e = jnp.exp2(s_t - m_new)
            alpha = jnp.exp2(m_old - m_new)
            m_st[g, 0:1, ls] = m_new
            l_st[g, 0:1, ls] = l_st[g, 0:1, ls] * alpha + jnp.sum(e, axis=0, keepdims=True)
            rows = slice(kvw + g * head_dim, kvw + (g + 1) * head_dim)
            pv = jnp.dot(kvt[rows, :n_k], e.astype(BF16), preferred_element_type=F32)
            oacc[g, :, ls] = oacc[g, :, ls] * alpha + pv

    def tile_of(dist):
        return lax.rem(z + dist + n_chip, n_chip) * 2 + c

    far = n_chip // 2

    def serve(part, dist):
        lo, hi = tile_of(-dist), tile_of(dist)
        if dist == far:
            for dirn in (UP, DN):
                far_copy(dirn, hi, part).wait_recv()
            ring_copy(D2D, hi, part).start()
            return
        for dirn, tile in ((UP, lo), (DN, hi)):
            ring_copy(dirn, tile, part).wait_recv()
            if dist < far - 1:
                ring_copy(dirn, tile, part).start()
            else:
                far_copy(dirn, tile, part).start()
            ring_copy(D2D, tile, part).start()

    plan = {1: [(0, 1), (1, 1)]}
    for d in range(2, far):
        plan[2 * d - 2] = [(0, d)]
        plan[2 * d - 1] = [(1, d)]
    plan[2 * far - 2] = [(0, far), (1, far)]

    def layer(l, carry):
        has_next = l + 1 < n_layers

        norm_rows(gains[0, l, 0:1, :], 0, n_tok)

        @pl.when(l > 0)
        def _():
            for i in range(3):
                pl.semaphore_wait(cred.at[i], 1)

        for part in range(2):
            a_copy(l, part).wait()
            ts = project(ring_a.at[a_slot(l, part)])
            if part == 0:
                for n, b in enumerate(rope_t(ts[0]) + rope_t(ts[1])):
                    kv[me, n * half:(n + 1) * half, :] = b.astype(BF16)
            else:
                kv[me, kvw:kvw + kvw // 2, :] = ts[0].astype(BF16)
                kv[me, kvw + kvw // 2:2 * kvw, :] = ts[1].astype(BF16)
            for dirn in (UP, DN, D2D):
                ring_copy(dirn, me, part).start()
            a_refill(l, part)

        @pl.when(l == 0)
        def _():
            for q in range(ahead_b):
                for t in range(2):
                    (up_copy(0, q, t) if q < n_up else dn_copy(0, q - n_up, t)).start()

        for i0 in range(0, n_q, 2):
            for i in (i0, i0 + 1):
                a_copy(l, first_q + i).wait()
            for i in (i0, i0 + 1):
                ts = project(ring_a.at[a_slot(l, first_q + i)])
                outs = [(b.astype(BF16).astype(F32) * head_dim ** -0.5).astype(BF16) for b in rope_t(ts[0]) + rope_t(ts[1])]
                n_g = rows_a // (q_group * head_dim)
                for gg in range(n_g):
                    g = i * n_g + gg
                    for hb in range(2):
                        parts = [outs[2 * (gg * q_group + hh) + hb] for hh in range(q_group)]
                        r0 = (g % 2) * head_dim + hb * half
                        qx[g, r0:r0 + half, :lane_f] = fronts(parts)
                        qx[g, r0:r0 + half, lane_f:] = backs(parts)
            for i in (i0, i0 + 1):
                a_refill(l, first_q + i)

        m_st[...] = jnp.full_like(m_st, MASK_FILL * LOG2E)
        l_st[...] = jnp.zeros_like(l_st)
        oacc[...] = jnp.zeros_like(oacc)

        for part in range(2):
            ring_copy(D2D, partner, part).wait_recv()
        attend(z, [(0, 1), (1, 2)])

        def step(k, carry):
            dist = (k + 1) // 2
            for at, todo in plan.items():
                @pl.when(k == at)
                def _():
                    for part, d in todo:
                        serve(part, d)
            chip = jnp.where(k % 2 == 1, z - dist + n_chip, z + dist) % n_chip
            other = chip * 2 + 1 - c
            for part in range(2):
                ring_copy(D2D, other, part).wait_recv()

            @pl.when(chip < z)
            def _():
                attend(chip, [(0, 1), (1, 1)])

            @pl.when(chip > z)
            def _():
                attend(chip, [(1, 2)])

            return carry

        lax.fori_loop(1, n_chip, step, 0)

        ck = pltpu.make_async_copy(cbuf.at[0], kc.at[l], csem.at[0])
        cv = pltpu.make_async_copy(cbuf.at[1], vc.at[l], csem.at[1])
        ck.start()
        cv.start()

        for i in range(n_o):
            a_copy(l, first_o + i).wait()
        y = None
        for i in range(n_o):
            n_g = rows_a // (q_group * head_dim)
            parts = []
            for gg in range(n_g):
                g = i * n_g + gg
                o = oacc[g] * (1.0 / l_st[g, 0:1, :])
                for hh in range(q_group):
                    f0 = hh * half_tok
                    parts.append(jnp.concatenate(
                        [o[:, f0:f0 + half_tok], o[:, lane_f + f0:lane_f + f0 + half_tok]], axis=1))
            o_n[:, i * rows_a:(i + 1) * rows_a] = jnp.concatenate(parts, axis=0).T.astype(BF16)
        for j in range(n_dn):
            cols = slice(j * cols_b, (j + 1) * cols_b)
            y = None
            for i in range(n_o):
                t = jnp.dot(o_n[:, i * rows_a:(i + 1) * rows_a], ring_a[a_slot(l, first_o + i), :, cols], preferred_element_type=F32)
                y = t if y is None else y + t
            acc[:, cols] = y
        for i in range(n_o):
            a_refill(l, first_o + i)

        gain = gains[1, l, 0:1, :]
        for i in range(2):
            def one(r, carry):
                rows = pl.ds(pl.multiple_of(i * half_tok + r * blk, blk), blk)
                xs[rows, :] = (xs[rows, :].astype(F32) + acc[rows, :]).astype(BF16)
                return carry

            lax.fori_loop(0, half_tok // blk, one, 0, unroll=2)
            norm_rows(gain, i * half_tok, half_tok)
            h_copy(i).start()

        ck.wait()
        cv.wait()
        for part in range(2):
            for dirn in (UP, DN, D2D):
                ring_copy(dirn, me, part).wait_send()
            for dist in range(1, far):
                for dirn, tile in ((UP, tile_of(-dist)), (DN, tile_of(dist))):
                    if dist < far - 1:
                        ring_copy(dirn, tile, part).wait_send()
                    else:
                        far_copy(dirn, tile, part).wait_send()
                    ring_copy(D2D, tile, part).wait_send()
            ring_copy(D2D, tile_of(far), part).wait_send()

        @pl.when(has_next)
        def _():
            pl.semaphore_signal(cred.at[DN], inc=1, device_id={"cp": up}, device_id_type=MESH)
            pl.semaphore_signal(cred.at[UP], inc=1, device_id={"cp": dn}, device_id_type=MESH)
            pl.semaphore_signal(cred.at[D2D], inc=1, device_id={"cp": partner}, device_id_type=MESH)

        for i in range(2):
            h_copy(i).wait_recv()

        def up_step(j0, carry):
            js = (2 * j0, 2 * j0 + 1)
            for j in js:
                for t in range(2):
                    up_copy(l, j, t).wait()
            h_all = h2[...].reshape(2 * n_tok, d_model)
            for j in js:
                a = jnp.dot(h_all, ring_b[b_slot(l, j, 0)], preferred_element_type=F32)
                b = jnp.dot(h_all, ring_b[b_slot(l, j, 1)], preferred_element_type=F32)
                ub[:, pl.ds(pl.multiple_of(j * cols_b, cols_b), cols_b)] = (jax.nn.silu(a) * b).astype(BF16)
            for j in js:
                b_refill(l, j)
            return carry

        lax.fori_loop(0, n_up // 2, up_step, 0)

        def dn_step(n, carry):
            for t in range(2):
                dn_copy(l, n, t).wait()
            y = jnp.dot(ub[:, :k_b], ring_b[b_slot(l, n_up + n, 0)], preferred_element_type=F32)
            y += jnp.dot(ub[:, k_b:], ring_b[b_slot(l, n_up + n, 1)], preferred_element_type=F32)
            psend[n] = y[n_tok:]
            p_copy(n).start()
            acc[:, pl.ds(pl.multiple_of(n * cols_b, cols_b), cols_b)] = y[:n_tok]
            b_refill(l, n_up + n)
            return carry

        lax.fori_loop(0, n_dn, dn_step, 0)
        for i in range(2):
            h_copy(i).wait_send()

        def merge(n, carry):
            p_copy(n).wait()
            cols = pl.ds(pl.multiple_of(n * cols_b, cols_b), cols_b)
            xs[:, cols] = (xs[:, cols].astype(F32) + (acc[:, cols] + precv[n])).astype(BF16)
            return carry

        lax.fori_loop(0, n_dn, merge, 0)
        return carry

    lax.fori_loop(0, n_layers, layer, 0)
    x_out[...] = xs[...]


def solution(mesh):
    n_cp = mesh.shape["cp"]
    row_spec = P(("req", "cp"), None)
    tok_spec = P(("req", "cp"))
    rep_spec = P()
    cache_spec = P(None, "req", "cp")

    def local_step(hidden, positions, segments, gain_1, gain_2, w_q, w_k, w_v, w_o, w_1, w_3, w_2):
        n_layers, d_model, n_heads, head_dim = w_q.shape
        n_kv = w_k.shape[2]
        n_tok = hidden.shape[0]
        kvw = n_kv * head_dim
        q_group = n_heads // n_kv
        d_ff = w_1.shape[2]
        rows_a, cols_b, k_b, nb = kvw, d_model // 4, d_ff // 4, NB
        inv_freq = ROPE_THETA ** (-2.0 * jnp.arange(head_dim // 2, dtype=F32) / head_dim)
        angle = inv_freq[:, None] * positions.astype(F32)[None, :]
        cos_t, sin_t = jnp.cos(angle), jnp.sin(angle)
        pos_2 = positions.reshape(2, n_tok // 2)
        pos_2 = jnp.concatenate([pos_2, pos_2], axis=1)

        def turned(w):
            return jnp.transpose(w, (0, 2, 3, 1)).reshape(n_layers, -1, d_model)

        cfg = dict(layers=n_layers, n_cp=n_cp, nb=nb)
        vmem = pl.BlockSpec(memory_space=pltpu.VMEM)
        hbm = pl.BlockSpec(memory_space=pl.ANY)
        n_all = n_cp * n_tok
        cache = jax.ShapeDtypeStruct((n_layers, kvw // n_cp, n_all), BF16)
        x, k_c, v_c = pl.pallas_call(
            functools.partial(kernel, cfg),
            out_shape=(jax.ShapeDtypeStruct(hidden.shape, BF16), cache, cache),
            in_specs=[vmem] * 6 + [hbm] * 7,
            out_specs=(vmem, hbm, hbm),
            scratch_shapes=[
                pltpu.VMEM((NA, rows_a, d_model), BF16),
                pltpu.VMEM((nb, k_b, cols_b), BF16),
                pltpu.VMEM((n_cp, 2 * kvw, n_tok), BF16),
                pltpu.VMEM((2 * kvw, 2 * n_tok), BF16),
                pltpu.VMEM((n_kv // 2, 2 * n_tok, 2 * head_dim), BF16),
                pltpu.VMEM((n_kv, 2 * head_dim, q_group * n_tok), BF16),
                pltpu.VMEM((n_kv, head_dim, q_group * n_tok), F32),
                pltpu.VMEM((n_kv, 8, q_group * n_tok), F32),
                pltpu.VMEM((n_kv, 8, q_group * n_tok), F32),
                pltpu.VMEM((2, 2 * n_tok, n_tok), F32),
                pltpu.VMEM((2, kvw // n_cp, n_all), BF16),
                pltpu.VMEM((n_tok, n_heads * head_dim), BF16),
                pltpu.VMEM((n_tok, d_model), BF16),
                pltpu.VMEM((2, n_tok, d_model), BF16),
                pltpu.VMEM((2 * n_tok, d_ff // 2), BF16),
                pltpu.VMEM((n_tok, d_model), F32),
                pltpu.VMEM((d_model // cols_b, n_tok, cols_b), F32),
                pltpu.VMEM((d_model // cols_b, n_tok, cols_b), F32),
                pltpu.VMEM((2, n_layers, 8, d_model), F32),
                pltpu.SemaphoreType.DMA((NA,)),
                pltpu.SemaphoreType.DMA((nb,)),
                pltpu.SemaphoreType.DMA((3, n_cp, 2)),
                pltpu.SemaphoreType.DMA((n_cp, 2)),
                pltpu.SemaphoreType.DMA((2, 2)),
                pltpu.SemaphoreType.DMA((2, 2)),
                pltpu.SemaphoreType.DMA((2,)),
                pltpu.SemaphoreType.DMA((2,)),
                pltpu.SemaphoreType.DMA((d_model // cols_b,)),
                pltpu.SemaphoreType.DMA((d_model // cols_b,)),
                pltpu.SemaphoreType.REGULAR((3,)),
                pltpu.SemaphoreType.DMA((2,)),
            ],
            compiler_params=pltpu.CompilerParams(
                collective_id=0, has_side_effects=True, vmem_limit_bytes=67043328),
            name="prefill",
        )(
            hidden, pos_2, cos_t, sin_t, gain_1, gain_2,
            turned(w_q), turned(w_k), turned(w_v), w_o.reshape(n_layers, -1, d_model), w_1, w_3, w_2,
        )
        return x, jnp.transpose(k_c, (0, 2, 1)), jnp.transpose(v_c, (0, 2, 1))

    return jax.shard_map(
        local_step,
        mesh=mesh,
        in_specs=(row_spec, tok_spec, tok_spec) + (rep_spec,) * 9,
        out_specs=(row_spec, cache_spec, cache_spec),
        check_vma=False,
    )
```

```python
import functools
import math

import jax
import jax.numpy as jnp
from jax import lax
from jax.experimental import pallas as pl
from jax.experimental.pallas import tpu as pltpu
from jax.sharding import PartitionSpec as P

NORM_EPS = 1e-5
ROPE_THETA = 10000.0
MASK_FILL = -1e30
BIG = 3e38
LOG2E = math.log2(math.e)
MESH = pl.DeviceIdType.MESH
F32 = jnp.float32
BF16 = jnp.bfloat16
NT = (((1,), (1,)), ((), ()))
NA = 4
NB = 16
AHEAD = 2
UP, DN, D2D = 0, 1, 2


def kernel(cfg, x_in, pos_in, cos_in, sin_in, g1_in, g2_in, wq, wk, wv, wo, w1, w3, w2,
           x_out, kc, vc,
           ring_a, ring_b, kv, kvt, knat, qx, oacc, m_st, l_st, cap, cbuf, o_n, xs, h2, ub, acc, psend, precv, gains,
           sem_a, sem_b, send_sem, recv_sem, fs_sem, fr_sem, hs_sem, hr_sem, ps_sem, pr_sem, cred, csem):
    n_layers, n_cp, nb = cfg["layers"], cfg["n_cp"], cfg["nb"]
    n_tok, d_model = xs.shape
    half_tok = n_tok // 2
    n_chip = n_cp // 2
    n_kv, head_dim, lanes = oacc.shape
    q_group = lanes // n_tok
    lane_f = lanes // 2
    kvw = n_kv * head_dim
    half = head_dim // 2
    rows_a = ring_a.shape[1]
    k_b, cols_b = ring_b.shape[1:]
    own_ff = ub.shape[1]
    n_up = own_ff // cols_b
    n_dn = d_model // cols_b
    n_kh = own_ff // k_b
    n_pair = n_up + n_dn
    ahead_b = nb // 2
    n_q = wq.shape[1] // rows_a
    n_o = wo.shape[1] // rows_a
    n_pos = 2 + n_q + n_o
    first_q, first_o = 2, 2 + n_q
    n_col = kvw // n_cp

    me = lax.axis_index("cp")
    z, c = me // 2, me % 2
    up = ((z + 1) % n_chip) * 2 + c
    dn = ((z + n_chip - 1) % n_chip) * 2 + c
    partner = z * 2 + (1 - c)

    def a_slot(l, pos):
        return lax.rem(l * n_pos + pos, NA)

    def a_copy(l, pos):
        if pos >= n_pos:
            l, pos = l + 1, pos - n_pos
        slot = a_slot(l, pos)
        if pos == 0:
            src = wk.at[l]
        elif pos == 1:
            src = wv.at[l]
        elif pos < first_o:
            src = wq.at[l, pl.ds((pos - first_q) * rows_a, rows_a), :]
        else:
            src = wo.at[l, pl.ds((pos - first_o) * rows_a, rows_a), :]
        return pltpu.make_async_copy(src, ring_a.at[slot], sem_a.at[slot])

    def a_refill(l, pos):
        if pos + NA < n_pos:
            a_copy(l, pos + NA).start()
        else:
            @pl.when(l + 1 < n_layers)
            def _():
                a_copy(l, pos + NA).start()

    def b_slot(l, q, t):
        return lax.rem((l * n_pair + q) * 2 + t, nb)

    def up_copy(l, j, t):
        slot = b_slot(l, j, t)
        col = pl.multiple_of(c * own_ff + j * cols_b, cols_b)
        return pltpu.make_async_copy((w1, w3)[t].at[l, :, pl.ds(col, cols_b)], ring_b.at[slot], sem_b.at[slot])

    def dn_copy(l, n, t):
        slot = b_slot(l, n_up + n, t)
        row = pl.multiple_of(c * own_ff + t * k_b, k_b)
        col = pl.multiple_of(n * cols_b, cols_b)
        return pltpu.make_async_copy(w2.at[l, pl.ds(row, k_b), pl.ds(col, cols_b)], ring_b.at[slot], sem_b.at[slot])

    def b_refill(l, q):
        q2 = q + ahead_b
        l2 = l + q2 // n_pair
        q3 = lax.rem(q2, n_pair)

        @pl.when((l2 < n_layers) & (q3 < n_up))
        def _():
            for t in range(2):
                up_copy(l2, q3, t).start()

        @pl.when((l2 < n_layers) & (q3 >= n_up))
        def _():
            for t in range(2):
                dn_copy(l2, q3 - n_up, t).start()

    def ring_copy(dirn, tile, part):
        ref = kv.at[tile, pl.ds(part * kvw, kvw), :]
        dev = (up, dn, partner)[dirn]
        return pltpu.make_async_remote_copy(
            src_ref=ref, dst_ref=ref, send_sem=send_sem.at[dirn, tile, part],
            recv_sem=recv_sem.at[tile, part], device_id={"cp": dev}, device_id_type=MESH)

    def far_copy(dirn, tile, part):
        ref = kv.at[tile, pl.ds(part * kvw + dirn * (kvw // 2), kvw // 2), :]
        return pltpu.make_async_remote_copy(
            src_ref=ref, dst_ref=ref, send_sem=fs_sem.at[dirn, part],
            recv_sem=fr_sem.at[dirn, part], device_id={"cp": (up, dn)[dirn]}, device_id_type=MESH)

    def h_copy(i):
        rows = pl.ds(i * half_tok, half_tok)
        return pltpu.make_async_remote_copy(
            src_ref=h2.at[0, rows, :], dst_ref=h2.at[1, rows, :], send_sem=hs_sem.at[i],
            recv_sem=hr_sem.at[i], device_id={"cp": partner}, device_id_type=MESH)

    def p_copy(n):
        return pltpu.make_async_remote_copy(
            src_ref=psend.at[n], dst_ref=precv.at[n], send_sem=ps_sem.at[n],
            recv_sem=pr_sem.at[n], device_id={"cp": partner}, device_id_type=MESH)

    pltpu.make_async_copy(x_in, xs, csem.at[0]).start()
    for pos in range(NA):
        a_copy(0, pos).start()
    barrier = pltpu.get_barrier_semaphore()
    for dev in (up, dn, partner):
        pl.semaphore_signal(barrier, inc=1, device_id={"cp": dev}, device_id_type=MESH)

    qx[...] = jnp.zeros_like(qx)
    for i in range(n_layers):
        gains[0, i, 0:1, :] = g1_in[i:i + 1, :].astype(F32)
        gains[1, i, 0:1, :] = g2_in[i:i + 1, :].astype(F32)
    pl.semaphore_wait(barrier, 3)
    pltpu.make_async_copy(x_in, xs, csem.at[0]).wait()

    blk = 16

    def norm_rows(gain, first, count):
        def one(r, carry):
            rows = pl.ds(pl.multiple_of(first + r * blk, blk), blk)
            v = xs[rows, :].astype(F32)
            inv = lax.rsqrt(jnp.mean(v * v, axis=-1, keepdims=True) + NORM_EPS)
            h2[0, rows, :] = (v * inv * gain).astype(BF16)
            return carry

        lax.fori_loop(0, count // blk, one, 0, unroll=2)

    def rope_t(t):
        cos_b = cos_in[...]
        sin_b = sin_in[...]
        outs = []
        for n in range(t.shape[0] // head_dim):
            a = t[n * head_dim:n * head_dim + half]
            b = t[n * head_dim + half:(n + 1) * head_dim]
            outs.append(a * cos_b - b * sin_b)
            outs.append(b * cos_b + a * sin_b)
        return outs

    def project(ref):
        mid = rows_a // 2
        return [lax.dot_general(ref[i * mid:(i + 1) * mid, :], h2[0], NT, preferred_element_type=F32) for i in range(2)]

    def fronts(parts):
        return jnp.concatenate([p[:, :half_tok] for p in parts], axis=1)

    def backs(parts):
        return jnp.concatenate([p[:, half_tok:] for p in parts], axis=1)

    n_unit = 2 * n_chip
    lane = lax.rem(lax.broadcasted_iota(jnp.int32, (1, n_tok), 1), half_tok)
    nat_qs = (me * half_tok + lane, (2 * n_cp - 1 - me) * half_tok + lane)

    def retile(chip):
        step_r = 256
        for r in range(0, 2 * kvw, step_r):
            t0 = kv[chip * 2, r:r + step_r, :]
            t1 = kv[chip * 2 + 1, r:r + step_r, :]
            kvt[r:r + step_r, :n_tok] = fronts([t0, t1])
            kvt[r:r + step_r, n_tok:] = backs([t1, t0])

    def cache_cols(chip):
        r0 = pl.multiple_of(me * n_col, n_col)
        for t in range(2):
            rows = kvt[pl.ds(t * kvw + r0, n_col), :]
            cbuf[t, :, pl.ds(pl.multiple_of(chip * n_tok, n_tok), n_tok)] = rows[:, :n_tok]
            cbuf[t, :, pl.ds(pl.multiple_of((n_unit - 1 - chip) * n_tok, n_tok), n_tok)] = rows[:, n_tok:]

    def attend(chip, blocks):
        retile(chip)
        cache_cols(chip)
        units = max(u for _, u in blocks)
        for p in range(n_kv // 2):
            rows = slice(p * 2 * head_dim, (p + 1) * 2 * head_dim)
            for u in range(units):
                knat[p, u * n_tok:(u + 1) * n_tok, :] = kvt[rows, u * n_tok:(u + 1) * n_tok].T
        key = lax.broadcasted_iota(jnp.int32, (n_tok, n_tok), 0)
        for qh, n_u in blocks:
            pos_q = pos_in[:, qh * half_tok:(qh + 1) * half_tok]
            start_q = nat_qs[qh] - jnp.concatenate([pos_q, pos_q], axis=1)
            for u in range(n_u):
                nat_k = (chip if u == 0 else n_unit - 1 - chip) * n_tok + key
                ok = (nat_k >= start_q) & (nat_k <= nat_qs[qh])
                cap[qh, u * n_tok:(u + 1) * n_tok, :] = jnp.where(ok, BIG, MASK_FILL)

        jobs = [(g, qh, n_u * n_tok) for g in range(n_kv) for qh, n_u in blocks]

        def scores(g, qh, n_k):
            return jnp.dot(knat[g // 2, :n_k, :], qx[g, :, qh * lane_f:(qh + 1) * lane_f], preferred_element_type=F32)

        ahead = [scores(*job) for job in jobs[:AHEAD]]
        for n, (g, qh, n_k) in enumerate(jobs):
            ls = slice(qh * lane_f, (qh + 1) * lane_f)
            capv = cap[qh, :n_k, :]
            capv = jnp.concatenate([capv] * (lane_f // n_tok), axis=1)
            s_t = jnp.minimum(ahead.pop(0), capv) * LOG2E
            if n + AHEAD < len(jobs):
                ahead.append(scores(*jobs[n + AHEAD]))
            m_old = m_st[g, 0:1, ls]
            m_new = jnp.maximum(m_old, jnp.max(s_t, axis=0, keepdims=True))
            e = jnp.exp2(s_t - m_new)
            alpha = jnp.exp2(m_old - m_new)
            m_st[g, 0:1, ls] = m_new
            l_st[g, 0:1, ls] = l_st[g, 0:1, ls] * alpha + jnp.sum(e, axis=0, keepdims=True)
            rows = slice(kvw + g * head_dim, kvw + (g + 1) * head_dim)
            pv = jnp.dot(kvt[rows, :n_k], e.astype(BF16), preferred_element_type=F32)
            oacc[g, :, ls] = oacc[g, :, ls] * alpha + pv

    def tile_of(dist):
        return lax.rem(z + dist + n_chip, n_chip) * 2 + c

    far = n_chip // 2

    def serve(part, dist):
        lo, hi = tile_of(-dist), tile_of(dist)
        if dist == far:
            for dirn in (UP, DN):
                far_copy(dirn, hi, part).wait_recv()
            ring_copy(D2D, hi, part).start()
            return
        for dirn, tile in ((UP, lo), (DN, hi)):
            ring_copy(dirn, tile, part).wait_recv()
            if dist < far - 1:
                ring_copy(dirn, tile, part).start()
            else:
                far_copy(dirn, tile, part).start()
            ring_copy(D2D, tile, part).start()

    plan = {1: [(0, 1), (1, 1)]}
    for d in range(2, far):
        plan[2 * d - 2] = [(0, d)]
        plan[2 * d - 1] = [(1, d)]
    plan[2 * far - 2] = [(0, far), (1, far)]

    def layer(l, carry):
        has_next = l + 1 < n_layers

        norm_rows(gains[0, l, 0:1, :], 0, n_tok)

        @pl.when(l > 0)
        def _():
            for i in range(3):
                pl.semaphore_wait(cred.at[i], 1)

        for part in range(2):
            a_copy(l, part).wait()
            ts = project(ring_a.at[a_slot(l, part)])
            if part == 0:
                for n, b in enumerate(rope_t(ts[0]) + rope_t(ts[1])):
                    kv[me, n * half:(n + 1) * half, :] = b.astype(BF16)
            else:
                kv[me, kvw:kvw + kvw // 2, :] = ts[0].astype(BF16)
                kv[me, kvw + kvw // 2:2 * kvw, :] = ts[1].astype(BF16)
            for dirn in (UP, DN, D2D):
                ring_copy(dirn, me, part).start()
            a_refill(l, part)

        @pl.when(l == 0)
        def _():
            for q in range(ahead_b):
                for t in range(2):
                    (up_copy(0, q, t) if q < n_up else dn_copy(0, q - n_up, t)).start()

        for i0 in range(0, n_q, 2):
            for i in (i0, i0 + 1):
                a_copy(l, first_q + i).wait()
            for i in (i0, i0 + 1):
                ts = project(ring_a.at[a_slot(l, first_q + i)])
                outs = [(b.astype(BF16).astype(F32) * head_dim ** -0.5).astype(BF16) for b in rope_t(ts[0]) + rope_t(ts[1])]
                n_g = rows_a // (q_group * head_dim)
                for gg in range(n_g):
                    g = i * n_g + gg
                    for hb in range(2):
                        parts = [outs[2 * (gg * q_group + hh) + hb] for hh in range(q_group)]
                        r0 = (g % 2) * head_dim + hb * half
                        qx[g, r0:r0 + half, :lane_f] = fronts(parts)
                        qx[g, r0:r0 + half, lane_f:] = backs(parts)
            for i in (i0, i0 + 1):
                a_refill(l, first_q + i)

        m_st[...] = jnp.full_like(m_st, MASK_FILL * LOG2E)
        l_st[...] = jnp.zeros_like(l_st)
        oacc[...] = jnp.zeros_like(oacc)

        for part in range(2):
            ring_copy(D2D, partner, part).wait_recv()
        attend(z, [(0, 1), (1, 2)])

        def step(k, carry):
            dist = (k + 1) // 2
            for at, todo in plan.items():
                @pl.when(k == at)
                def _():
                    for part, d in todo:
                        serve(part, d)
            chip = jnp.where(k % 2 == 1, z - dist + n_chip, z + dist) % n_chip
            other = chip * 2 + 1 - c
            for part in range(2):
                ring_copy(D2D, other, part).wait_recv()

            @pl.when(chip < z)
            def _():
                attend(chip, [(0, 1), (1, 1)])

            @pl.when(chip > z)
            def _():
                attend(chip, [(1, 2)])

            return carry

        lax.fori_loop(1, n_chip, step, 0)

        ck = pltpu.make_async_copy(cbuf.at[0], kc.at[l], csem.at[0])
        cv = pltpu.make_async_copy(cbuf.at[1], vc.at[l], csem.at[1])
        ck.start()
        cv.start()

        for i in range(n_o):
            a_copy(l, first_o + i).wait()
        y = None
        for i in range(n_o):
            n_g = rows_a // (q_group * head_dim)
            parts = []
            for gg in range(n_g):
                g = i * n_g + gg
                o = oacc[g] * (1.0 / l_st[g, 0:1, :])
                for hh in range(q_group):
                    f0 = hh * half_tok
                    parts.append(jnp.concatenate(
                        [o[:, f0:f0 + half_tok], o[:, lane_f + f0:lane_f + f0 + half_tok]], axis=1))
            o_n[:, i * rows_a:(i + 1) * rows_a] = jnp.concatenate(parts, axis=0).T.astype(BF16)
        for j in range(n_dn):
            cols = slice(j * cols_b, (j + 1) * cols_b)
            y = None
            for i in range(n_o):
                t = jnp.dot(o_n[:, i * rows_a:(i + 1) * rows_a], ring_a[a_slot(l, first_o + i), :, cols], preferred_element_type=F32)
                y = t if y is None else y + t
            acc[:, cols] = y
        for i in range(n_o):
            a_refill(l, first_o + i)

        gain = gains[1, l, 0:1, :]
        for i in range(2):
            def one(r, carry):
                rows = pl.ds(pl.multiple_of(i * half_tok + r * blk, blk), blk)
                xs[rows, :] = (xs[rows, :].astype(F32) + acc[rows, :]).astype(BF16)
                return carry

            lax.fori_loop(0, half_tok // blk, one, 0, unroll=2)
            norm_rows(gain, i * half_tok, half_tok)
            h_copy(i).start()

        ck.wait()
        cv.wait()
        for part in range(2):
            for dirn in (UP, DN, D2D):
                ring_copy(dirn, me, part).wait_send()
            for dist in range(1, far):
                for dirn, tile in ((UP, tile_of(-dist)), (DN, tile_of(dist))):
                    if dist < far - 1:
                        ring_copy(dirn, tile, part).wait_send()
                    else:
                        far_copy(dirn, tile, part).wait_send()
                    ring_copy(D2D, tile, part).wait_send()
            ring_copy(D2D, tile_of(far), part).wait_send()

        @pl.when(has_next)
        def _():
            pl.semaphore_signal(cred.at[DN], inc=1, device_id={"cp": up}, device_id_type=MESH)
            pl.semaphore_signal(cred.at[UP], inc=1, device_id={"cp": dn}, device_id_type=MESH)
            pl.semaphore_signal(cred.at[D2D], inc=1, device_id={"cp": partner}, device_id_type=MESH)

        def up_dots(h_rows, rows, js):
            for j in js:
                a = jnp.dot(h_rows, ring_b[b_slot(l, j, 0)], preferred_element_type=F32)
                b = jnp.dot(h_rows, ring_b[b_slot(l, j, 1)], preferred_element_type=F32)
                ub[rows, pl.ds(pl.multiple_of(j * cols_b, cols_b), cols_b)] = (jax.nn.silu(a) * b).astype(BF16)

        def up_step(j0, carry):
            js = (2 * j0, 2 * j0 + 1)
            for j in js:
                for t in range(2):
                    up_copy(l, j, t).wait()
            up_dots(h2[...].reshape(2 * n_tok, d_model), slice(None), js)
            for j in js:
                b_refill(l, j)
            return carry

        for t in range(2):
            up_copy(l, 0, t).wait()
            up_copy(l, 1, t).wait()
        up_dots(h2[0], slice(0, n_tok), (0, 1))
        for i in range(2):
            h_copy(i).wait_recv()
        up_dots(h2[1], slice(n_tok, None), (0, 1))
        for j in range(2):
            b_refill(l, j)
        lax.fori_loop(1, n_up // 2, up_step, 0)

        def dn_dots(rows, n):
            y = jnp.dot(ub[rows, :k_b], ring_b[b_slot(l, n_up + n, 0)], preferred_element_type=F32)
            return y + jnp.dot(ub[rows, k_b:], ring_b[b_slot(l, n_up + n, 1)], preferred_element_type=F32)

        def merge(n):
            p_copy(n).wait()
            cols = pl.ds(pl.multiple_of(n * cols_b, cols_b), cols_b)
            xs[:, cols] = (xs[:, cols].astype(F32) + (acc[:, cols] + precv[n])).astype(BF16)

        def dn_step(n, carry):
            for t in range(2):
                dn_copy(l, n, t).wait()
            y = dn_dots(slice(None), n)
            psend[n] = y[n_tok:]
            p_copy(n).start()
            acc[:, pl.ds(pl.multiple_of(n * cols_b, cols_b), cols_b)] = y[:n_tok]
            b_refill(l, n_up + n)

            @pl.when(n > 0)
            def _():
                merge(n - 1)

            return carry

        lax.fori_loop(0, n_dn - 1, dn_step, 0)

        n = n_dn - 1
        for t in range(2):
            dn_copy(l, n, t).wait()
        psend[n] = dn_dots(slice(n_tok, None), n)
        p_copy(n).start()
        acc[:, n * cols_b:] = dn_dots(slice(0, n_tok), n)
        b_refill(l, n_up + n)
        merge(n - 1)
        for i in range(2):
            h_copy(i).wait_send()
        merge(n)
        return carry

    lax.fori_loop(0, n_layers, layer, 0)
    out_copy = pltpu.make_async_copy(xs, x_out, csem.at[0])
    out_copy.start()
    out_copy.wait()


def hand_over(*refs):
    ins, outs, bufs, sem = refs[:3], refs[3:6], refs[6:9], refs[9]
    first = [pltpu.make_async_copy(ins[i], bufs[i], sem.at[i]) for i in range(3)]
    second = [pltpu.make_async_copy(bufs[i], outs[i], sem.at[i]) for i in range(3)]
    for copy in first:
        copy.start()
    for i in range(3):
        first[i].wait()
        second[i].start()
    for copy in second:
        copy.wait()


def solution(mesh):
    n_cp = mesh.shape["cp"]
    row_spec = P(("req", "cp"), None)
    tok_spec = P(("req", "cp"))
    rep_spec = P()
    cache_spec = P(None, "req", "cp")

    def local_step(hidden, positions, segments, gain_1, gain_2, w_q, w_k, w_v, w_o, w_1, w_3, w_2):
        n_layers, d_model, n_heads, head_dim = w_q.shape
        n_kv = w_k.shape[2]
        n_tok = hidden.shape[0]
        kvw = n_kv * head_dim
        q_group = n_heads // n_kv
        d_ff = w_1.shape[2]
        rows_a, cols_b, k_b, nb = kvw, d_model // 4, d_ff // 4, NB
        inv_freq = ROPE_THETA ** (-2.0 * jnp.arange(head_dim // 2, dtype=F32) / head_dim)
        angle = inv_freq[:, None] * positions.astype(F32)[None, :]
        cos_t, sin_t = jnp.cos(angle), jnp.sin(angle)

        def turned(w):
            return jnp.transpose(w, (0, 2, 3, 1)).reshape(n_layers, -1, d_model)

        cfg = dict(layers=n_layers, n_cp=n_cp, nb=nb)
        vmem = pl.BlockSpec(memory_space=pltpu.VMEM)
        hbm = pl.BlockSpec(memory_space=pl.ANY)
        n_all = n_cp * n_tok
        cache = jax.ShapeDtypeStruct((n_layers, kvw // n_cp, n_all), BF16)
        x, k_c, v_c = pl.pallas_call(
            functools.partial(kernel, cfg),
            out_shape=(jax.ShapeDtypeStruct(hidden.shape, BF16), cache, cache),
            in_specs=[hbm] + [vmem] * 5 + [hbm] * 7,
            out_specs=(hbm, hbm, hbm),
            scratch_shapes=[
                pltpu.VMEM((NA, rows_a, d_model), BF16),
                pltpu.VMEM((nb, k_b, cols_b), BF16),
                pltpu.VMEM((n_cp, 2 * kvw, n_tok), BF16),
                pltpu.VMEM((2 * kvw, 2 * n_tok), BF16),
                pltpu.VMEM((n_kv // 2, 2 * n_tok, 2 * head_dim), BF16),
                pltpu.VMEM((n_kv, 2 * head_dim, q_group * n_tok), BF16),
                pltpu.VMEM((n_kv, head_dim, q_group * n_tok), F32),
                pltpu.VMEM((n_kv, 8, q_group * n_tok), F32),
                pltpu.VMEM((n_kv, 8, q_group * n_tok), F32),
                pltpu.VMEM((2, 2 * n_tok, n_tok), F32),
                pltpu.VMEM((2, kvw // n_cp, n_all), BF16),
                pltpu.VMEM((n_tok, n_heads * head_dim), BF16),
                pltpu.VMEM((n_tok, d_model), BF16),
                pltpu.VMEM((2, n_tok, d_model), BF16),
                pltpu.VMEM((2 * n_tok, d_ff // 2), BF16),
                pltpu.VMEM((n_tok, d_model), F32),
                pltpu.VMEM((d_model // cols_b, n_tok, cols_b), F32),
                pltpu.VMEM((d_model // cols_b, n_tok, cols_b), F32),
                pltpu.VMEM((2, n_layers, 8, d_model), F32),
                pltpu.SemaphoreType.DMA((NA,)),
                pltpu.SemaphoreType.DMA((nb,)),
                pltpu.SemaphoreType.DMA((3, n_cp, 2)),
                pltpu.SemaphoreType.DMA((n_cp, 2)),
                pltpu.SemaphoreType.DMA((2, 2)),
                pltpu.SemaphoreType.DMA((2, 2)),
                pltpu.SemaphoreType.DMA((2,)),
                pltpu.SemaphoreType.DMA((2,)),
                pltpu.SemaphoreType.DMA((d_model // cols_b,)),
                pltpu.SemaphoreType.DMA((d_model // cols_b,)),
                pltpu.SemaphoreType.REGULAR((3,)),
                pltpu.SemaphoreType.DMA((2,)),
            ],
            compiler_params=pltpu.CompilerParams(
                collective_id=0, has_side_effects=True, vmem_limit_bytes=67043328),
            name="prefill",
        )(
            hidden, positions[None, :], cos_t, sin_t, gain_1, gain_2,
            turned(w_q), turned(w_k), turned(w_v), w_o.reshape(n_layers, -1, d_model), w_1, w_3, w_2,
        )
        results = (x, k_c, v_c)
        x, k_c, v_c = pl.pallas_call(
            hand_over,
            out_shape=tuple(jax.ShapeDtypeStruct(r.shape, r.dtype) for r in results),
            in_specs=[hbm] * 3,
            out_specs=(hbm,) * 3,
            scratch_shapes=[pltpu.VMEM(r.shape, r.dtype) for r in results] + [pltpu.SemaphoreType.DMA((3,))],
            name="hand_over",
        )(*results)
        return x, jnp.transpose(k_c, (0, 2, 1)), jnp.transpose(v_c, (0, 2, 1))

    return jax.shard_map(
        local_step,
        mesh=mesh,
        in_specs=(row_spec, tok_spec, tok_spec) + (rep_spec,) * 9,
        out_specs=(row_spec, cache_spec, cache_spec),
        check_vma=False,
    )
```

```python
import functools
import math

import jax
import jax.numpy as jnp
from jax import lax
from jax.experimental import pallas as pl
from jax.experimental.pallas import tpu as pltpu
from jax.sharding import PartitionSpec as P

NORM_EPS = 1e-5
ROPE_THETA = 10000.0
MASK_FILL = -1e30
BIG = 3e38
LOG2E = math.log2(math.e)
MESH = pl.DeviceIdType.MESH
F32 = jnp.float32
BF16 = jnp.bfloat16
NT = (((1,), (1,)), ((), ()))
NA = 4
NB = 16
AHEAD = 2
UP, DN, D2D = 0, 1, 2


def kernel(cfg, x_in, pos_in, cos_in, sin_in, g1_in, g2_in, wq, wk, wv, wo, w1, w3, w2,
           x_out, kc, vc,
           ring_a, ring_b, kv, kvt, knat, qx, oacc, m_st, l_st, cap, cbuf, o_n, xs, h2, ub, acc, psend, precv, gains,
           sem_a, sem_b, send_sem, recv_sem, fs_sem, fr_sem, hs_sem, hr_sem, ps_sem, pr_sem, cred, csem):
    n_layers, n_cp, nb = cfg["layers"], cfg["n_cp"], cfg["nb"]
    n_tok, d_model = xs.shape
    half_tok = n_tok // 2
    n_chip = n_cp // 2
    n_kv, head_dim, lanes = oacc.shape
    q_group = lanes // n_tok
    lane_f = lanes // 2
    kvw = n_kv * head_dim
    half = head_dim // 2
    rows_a = ring_a.shape[1]
    k_b, cols_b = ring_b.shape[1:]
    own_ff = ub.shape[1]
    n_up = own_ff // cols_b
    n_dn = d_model // cols_b
    n_kh = own_ff // k_b
    n_pair = n_up + n_dn
    ahead_b = nb // 2
    n_q = wq.shape[1] // rows_a
    n_o = wo.shape[1] // rows_a
    n_pos = 2 + n_q + n_o
    first_q, first_o = 2, 2 + n_q
    n_col = kvw // n_cp

    me = lax.axis_index("cp")
    z, c = me // 2, me % 2
    up = ((z + 1) % n_chip) * 2 + c
    dn = ((z + n_chip - 1) % n_chip) * 2 + c
    partner = z * 2 + (1 - c)

    def a_slot(l, pos):
        return lax.rem(l * n_pos + pos, NA)

    def a_copy(l, pos):
        if pos >= n_pos:
            l, pos = l + 1, pos - n_pos
        slot = a_slot(l, pos)
        if pos == 0:
            src = wk.at[l]
        elif pos == 1:
            src = wv.at[l]
        elif pos < first_o:
            src = wq.at[l, pl.ds((pos - first_q) * rows_a, rows_a), :]
        else:
            src = wo.at[l, pl.ds((pos - first_o) * rows_a, rows_a), :]
        return pltpu.make_async_copy(src, ring_a.at[slot], sem_a.at[slot])

    def a_refill(l, pos):
        if pos + NA < n_pos:
            a_copy(l, pos + NA).start()
        else:
            @pl.when(l + 1 < n_layers)
            def _():
                a_copy(l, pos + NA).start()

    def b_slot(l, q, t):
        return lax.rem((l * n_pair + q) * 2 + t, nb)

    def up_copy(l, j, t):
        slot = b_slot(l, j, t)
        col = pl.multiple_of(c * own_ff + j * cols_b, cols_b)
        return pltpu.make_async_copy((w1, w3)[t].at[l, :, pl.ds(col, cols_b)], ring_b.at[slot], sem_b.at[slot])

    def dn_copy(l, n, t):
        slot = b_slot(l, n_up + n, t)
        row = pl.multiple_of(c * own_ff + t * k_b, k_b)
        col = pl.multiple_of(n * cols_b, cols_b)
        return pltpu.make_async_copy(w2.at[l, pl.ds(row, k_b), pl.ds(col, cols_b)], ring_b.at[slot], sem_b.at[slot])

    def b_refill(l, q):
        q2 = q + ahead_b
        l2 = l + q2 // n_pair
        q3 = lax.rem(q2, n_pair)

        @pl.when((l2 < n_layers) & (q3 < n_up))
        def _():
            for t in range(2):
                up_copy(l2, q3, t).start()

        @pl.when((l2 < n_layers) & (q3 >= n_up))
        def _():
            for t in range(2):
                dn_copy(l2, q3 - n_up, t).start()

    def ring_copy(dirn, tile, part):
        ref = kv.at[tile, pl.ds(part * kvw, kvw), :]
        dev = (up, dn, partner)[dirn]
        return pltpu.make_async_remote_copy(
            src_ref=ref, dst_ref=ref, send_sem=send_sem.at[dirn, tile, part],
            recv_sem=recv_sem.at[tile, part], device_id={"cp": dev}, device_id_type=MESH)

    def far_copy(dirn, tile, part):
        ref = kv.at[tile, pl.ds(part * kvw + dirn * (kvw // 2), kvw // 2), :]
        return pltpu.make_async_remote_copy(
            src_ref=ref, dst_ref=ref, send_sem=fs_sem.at[dirn, part],
            recv_sem=fr_sem.at[dirn, part], device_id={"cp": (up, dn)[dirn]}, device_id_type=MESH)

    def h_copy(i):
        rows = pl.ds(i * half_tok, half_tok)
        return pltpu.make_async_remote_copy(
            src_ref=h2.at[0, rows, :], dst_ref=h2.at[1, rows, :], send_sem=hs_sem.at[i],
            recv_sem=hr_sem.at[i], device_id={"cp": partner}, device_id_type=MESH)

    def p_copy(n):
        return pltpu.make_async_remote_copy(
            src_ref=psend.at[n], dst_ref=precv.at[n], send_sem=ps_sem.at[n],
            recv_sem=pr_sem.at[n], device_id={"cp": partner}, device_id_type=MESH)

    pltpu.make_async_copy(x_in, xs, csem.at[0]).start()
    for pos in range(NA):
        a_copy(0, pos).start()
    barrier = pltpu.get_barrier_semaphore()
    for dev in (up, dn, partner):
        pl.semaphore_signal(barrier, inc=1, device_id={"cp": dev}, device_id_type=MESH)

    qx[...] = jnp.zeros_like(qx)
    for i in range(n_layers):
        gains[0, i, 0:1, :] = g1_in[i:i + 1, :].astype(F32)
        gains[1, i, 0:1, :] = g2_in[i:i + 1, :].astype(F32)
    pl.semaphore_wait(barrier, 3)
    pltpu.make_async_copy(x_in, xs, csem.at[0]).wait()

    blk = 16

    def norm_rows(gain, first, count):
        def one(r, carry):
            rows = pl.ds(pl.multiple_of(first + r * blk, blk), blk)
            v = xs[rows, :].astype(F32)
            inv = lax.rsqrt(jnp.mean(v * v, axis=-1, keepdims=True) + NORM_EPS)
            h2[0, rows, :] = (v * inv * gain).astype(BF16)
            return carry

        lax.fori_loop(0, count // blk, one, 0, unroll=2)

    def rope_t(t):
        cos_b = cos_in[...]
        sin_b = sin_in[...]
        outs = []
        for n in range(t.shape[0] // head_dim):
            a = t[n * head_dim:n * head_dim + half]
            b = t[n * head_dim + half:(n + 1) * head_dim]
            outs.append(a * cos_b - b * sin_b)
            outs.append(b * cos_b + a * sin_b)
        return outs

    def project(ref):
        mid = rows_a // 2
        return [lax.dot_general(ref[i * mid:(i + 1) * mid, :], h2[0], NT, preferred_element_type=F32) for i in range(2)]

    def fronts(parts):
        return jnp.concatenate([p[:, :half_tok] for p in parts], axis=1)

    def backs(parts):
        return jnp.concatenate([p[:, half_tok:] for p in parts], axis=1)

    n_unit = 2 * n_chip
    lane = lax.rem(lax.broadcasted_iota(jnp.int32, (1, n_tok), 1), half_tok)
    nat_qs = (me * half_tok + lane, (2 * n_cp - 1 - me) * half_tok + lane)

    def retile(chip, units):
        step_r = 256
        for r in range(0, 2 * kvw, step_r):
            t0 = kv[chip * 2, r:r + step_r, :]
            t1 = kv[chip * 2 + 1, r:r + step_r, :]
            kvt[r:r + step_r, :n_tok] = fronts([t0, t1])
            if units == 2:
                kvt[r:r + step_r, n_tok:] = backs([t1, t0])

    def cache_cols(chip):
        r0 = pl.multiple_of(me * n_col, n_col)
        for t in range(2):
            rows = pl.ds(t * kvw + r0, n_col)
            t0, t1 = kv[chip * 2, rows, :], kv[chip * 2 + 1, rows, :]
            cbuf[t, :, pl.ds(pl.multiple_of(chip * n_tok, n_tok), n_tok)] = fronts([t0, t1])
            cbuf[t, :, pl.ds(pl.multiple_of((n_unit - 1 - chip) * n_tok, n_tok), n_tok)] = backs([t1, t0])

    def attend(chip, blocks):
        units = max(u for _, u in blocks)
        retile(chip, units)
        cache_cols(chip)
        for p in range(n_kv // 2):
            rows = slice(p * 2 * head_dim, (p + 1) * 2 * head_dim)
            for u in range(units):
                knat[p, u * n_tok:(u + 1) * n_tok, :] = kvt[rows, u * n_tok:(u + 1) * n_tok].T
        key = lax.broadcasted_iota(jnp.int32, (n_tok, n_tok), 0)
        for qh, n_u in blocks:
            pos_q = pos_in[:, qh * half_tok:(qh + 1) * half_tok]
            start_q = nat_qs[qh] - jnp.concatenate([pos_q, pos_q], axis=1)
            for u in range(n_u):
                nat_k = (chip if u == 0 else n_unit - 1 - chip) * n_tok + key
                ok = (nat_k >= start_q) & (nat_k <= nat_qs[qh])
                cap[qh, u * n_tok:(u + 1) * n_tok, :] = jnp.where(ok, BIG, MASK_FILL)

        jobs = [(g, qh, n_u * n_tok) for g in range(n_kv) for qh, n_u in blocks]

        def scores(g, qh, n_k):
            return jnp.dot(knat[g // 2, :n_k, :], qx[g, :, qh * lane_f:(qh + 1) * lane_f], preferred_element_type=F32)

        lead = AHEAD * (2 if units == 1 else 1)
        ahead = [scores(*job) for job in jobs[:lead]]
        for n, (g, qh, n_k) in enumerate(jobs):
            ls = slice(qh * lane_f, (qh + 1) * lane_f)
            capv = cap[qh, :n_k, :]
            capv = jnp.concatenate([capv] * (lane_f // n_tok), axis=1)
            s_t = jnp.minimum(ahead.pop(0), capv) * LOG2E
            if n + lead < len(jobs):
                ahead.append(scores(*jobs[n + lead]))
            m_old = m_st[g, 0:1, ls]
            m_new = jnp.maximum(m_old, jnp.max(s_t, axis=0, keepdims=True))
            e = jnp.exp2(s_t - m_new)
            alpha = jnp.exp2(m_old - m_new)
            m_st[g, 0:1, ls] = m_new
            l_st[g, 0:1, ls] = l_st[g, 0:1, ls] * alpha + jnp.sum(e, axis=0, keepdims=True)
            rows = slice(kvw + g * head_dim, kvw + (g + 1) * head_dim)
            pv = jnp.dot(kvt[rows, :n_k], e.astype(BF16), preferred_element_type=F32)
            oacc[g, :, ls] = oacc[g, :, ls] * alpha + pv

    def tile_of(dist):
        return lax.rem(z + dist + n_chip, n_chip) * 2 + c

    far = n_chip // 2

    def serve(part, dist):
        lo, hi = tile_of(-dist), tile_of(dist)
        if dist == far:
            for dirn in (UP, DN):
                far_copy(dirn, hi, part).wait_recv()
            ring_copy(D2D, hi, part).start()
            return
        for dirn, tile in ((UP, lo), (DN, hi)):
            ring_copy(dirn, tile, part).wait_recv()
            if dist < far - 1:
                ring_copy(dirn, tile, part).start()
            else:
                far_copy(dirn, tile, part).start()
            ring_copy(D2D, tile, part).start()

    plan = {1: [(0, 1), (1, 1)]}
    for d in range(2, far):
        plan[2 * d - 2] = [(0, d)]
        plan[2 * d - 1] = [(1, d)]
    plan[2 * far - 2] = [(0, far), (1, far)]

    def layer(l, carry):
        has_next = l + 1 < n_layers

        norm_rows(gains[0, l, 0:1, :], 0, n_tok)

        @pl.when(l > 0)
        def _():
            for i in range(3):
                pl.semaphore_wait(cred.at[i], 1)

        for part in range(2):
            a_copy(l, part).wait()
            ts = project(ring_a.at[a_slot(l, part)])
            if part == 0:
                for n, b in enumerate(rope_t(ts[0]) + rope_t(ts[1])):
                    kv[me, n * half:(n + 1) * half, :] = b.astype(BF16)
            else:
                kv[me, kvw:kvw + kvw // 2, :] = ts[0].astype(BF16)
                kv[me, kvw + kvw // 2:2 * kvw, :] = ts[1].astype(BF16)
            for dirn in (UP, DN, D2D):
                ring_copy(dirn, me, part).start()
            a_refill(l, part)

        @pl.when(l == 0)
        def _():
            for q in range(ahead_b):
                for t in range(2):
                    (up_copy(0, q, t) if q < n_up else dn_copy(0, q - n_up, t)).start()

        for i0 in range(0, n_q, 2):
            for i in (i0, i0 + 1):
                a_copy(l, first_q + i).wait()
            for i in (i0, i0 + 1):
                ts = project(ring_a.at[a_slot(l, first_q + i)])
                outs = [(b.astype(BF16).astype(F32) * head_dim ** -0.5).astype(BF16) for b in rope_t(ts[0]) + rope_t(ts[1])]
                n_g = rows_a // (q_group * head_dim)
                for gg in range(n_g):
                    g = i * n_g + gg
                    for hb in range(2):
                        parts = [outs[2 * (gg * q_group + hh) + hb] for hh in range(q_group)]
                        r0 = (g % 2) * head_dim + hb * half
                        qx[g, r0:r0 + half, :lane_f] = fronts(parts)
                        qx[g, r0:r0 + half, lane_f:] = backs(parts)
            for i in (i0, i0 + 1):
                a_refill(l, first_q + i)

        m_st[...] = jnp.full_like(m_st, MASK_FILL * LOG2E)
        l_st[...] = jnp.zeros_like(l_st)
        oacc[...] = jnp.zeros_like(oacc)

        for part in range(2):
            ring_copy(D2D, partner, part).wait_recv()
        attend(z, [(0, 1), (1, 2)])

        def step(k, carry):
            dist = (k + 1) // 2
            for at, todo in plan.items():
                @pl.when(k == at)
                def _():
                    for part, d in todo:
                        serve(part, d)
            chip = jnp.where(k % 2 == 1, z - dist + n_chip, z + dist) % n_chip
            other = chip * 2 + 1 - c
            for part in range(2):
                ring_copy(D2D, other, part).wait_recv()

            @pl.when(chip < z)
            def _():
                attend(chip, [(0, 1), (1, 1)])

            @pl.when(chip > z)
            def _():
                attend(chip, [(1, 2)])

            return carry

        lax.fori_loop(1, n_chip, step, 0)

        ck = pltpu.make_async_copy(cbuf.at[0], kc.at[l], csem.at[0])
        cv = pltpu.make_async_copy(cbuf.at[1], vc.at[l], csem.at[1])
        ck.start()
        cv.start()

        for i in range(n_o):
            a_copy(l, first_o + i).wait()
        y = None
        for i in range(n_o):
            n_g = rows_a // (q_group * head_dim)
            parts = []
            for gg in range(n_g):
                g = i * n_g + gg
                o = oacc[g] * (1.0 / l_st[g, 0:1, :])
                for hh in range(q_group):
                    f0 = hh * half_tok
                    parts.append(jnp.concatenate(
                        [o[:, f0:f0 + half_tok], o[:, lane_f + f0:lane_f + f0 + half_tok]], axis=1))
            o_n[:, i * rows_a:(i + 1) * rows_a] = jnp.concatenate(parts, axis=0).T.astype(BF16)
        for j in range(n_dn):
            cols = slice(j * cols_b, (j + 1) * cols_b)
            y = None
            for i in range(n_o):
                t = jnp.dot(o_n[:, i * rows_a:(i + 1) * rows_a], ring_a[a_slot(l, first_o + i), :, cols], preferred_element_type=F32)
                y = t if y is None else y + t
            acc[:, cols] = y
        for i in range(n_o):
            a_refill(l, first_o + i)

        gain = gains[1, l, 0:1, :]
        for i in range(2):
            def one(r, carry):
                rows = pl.ds(pl.multiple_of(i * half_tok + r * blk, blk), blk)
                x_new = (xs[rows, :].astype(F32) + acc[rows, :]).astype(BF16)
                xs[rows, :] = x_new
                v = x_new.astype(F32)
                inv = lax.rsqrt(jnp.mean(v * v, axis=-1, keepdims=True) + NORM_EPS)
                h2[0, rows, :] = (v * inv * gain).astype(BF16)
                return carry

            lax.fori_loop(0, half_tok // blk, one, 0, unroll=2)
            h_copy(i).start()

        ck.wait()
        cv.wait()
        for part in range(2):
            for dirn in (UP, DN, D2D):
                ring_copy(dirn, me, part).wait_send()
            for dist in range(1, far):
                for dirn, tile in ((UP, tile_of(-dist)), (DN, tile_of(dist))):
                    if dist < far - 1:
                        ring_copy(dirn, tile, part).wait_send()
                    else:
                        far_copy(dirn, tile, part).wait_send()
                    ring_copy(D2D, tile, part).wait_send()
            ring_copy(D2D, tile_of(far), part).wait_send()

        @pl.when(has_next)
        def _():
            pl.semaphore_signal(cred.at[DN], inc=1, device_id={"cp": up}, device_id_type=MESH)
            pl.semaphore_signal(cred.at[UP], inc=1, device_id={"cp": dn}, device_id_type=MESH)
            pl.semaphore_signal(cred.at[D2D], inc=1, device_id={"cp": partner}, device_id_type=MESH)

        def up_dots(h_rows, rows, js):
            for j in js:
                a = jnp.dot(h_rows, ring_b[b_slot(l, j, 0)], preferred_element_type=F32)
                b = jnp.dot(h_rows, ring_b[b_slot(l, j, 1)], preferred_element_type=F32)
                ub[rows, pl.ds(pl.multiple_of(j * cols_b, cols_b), cols_b)] = (jax.nn.silu(a) * b).astype(BF16)

        def up_step(j0, carry):
            js = (2 * j0, 2 * j0 + 1)
            for j in js:
                for t in range(2):
                    up_copy(l, j, t).wait()
            up_dots(h2[...].reshape(2 * n_tok, d_model), slice(None), js)
            for j in js:
                b_refill(l, j)
            return carry

        for t in range(2):
            up_copy(l, 0, t).wait()
            up_copy(l, 1, t).wait()
        up_dots(h2[0], slice(0, n_tok), (0, 1))
        for i in range(2):
            h_copy(i).wait_recv()
        up_dots(h2[1], slice(n_tok, None), (0, 1))
        for j in range(2):
            b_refill(l, j)
        lax.fori_loop(1, n_up // 2, up_step, 0)

        def dn_dots(rows, n):
            y = jnp.dot(ub[rows, :k_b], ring_b[b_slot(l, n_up + n, 0)], preferred_element_type=F32)
            return y + jnp.dot(ub[rows, k_b:], ring_b[b_slot(l, n_up + n, 1)], preferred_element_type=F32)

        def merge(n):
            p_copy(n).wait()
            cols = pl.ds(pl.multiple_of(n * cols_b, cols_b), cols_b)
            xs[:, cols] = (xs[:, cols].astype(F32) + (acc[:, cols] + precv[n])).astype(BF16)

        def dn_step(n, carry):
            for t in range(2):
                dn_copy(l, n, t).wait()
            y = dn_dots(slice(None), n)
            psend[n] = y[n_tok:]
            p_copy(n).start()
            acc[:, pl.ds(pl.multiple_of(n * cols_b, cols_b), cols_b)] = y[:n_tok]
            b_refill(l, n_up + n)

            @pl.when(n > 0)
            def _():
                merge(n - 1)

            return carry

        lax.fori_loop(0, n_dn - 1, dn_step, 0)

        n = n_dn - 1
        for t in range(2):
            dn_copy(l, n, t).wait()
        psend[n] = dn_dots(slice(n_tok, None), n)
        p_copy(n).start()
        acc[:, n * cols_b:] = dn_dots(slice(0, n_tok), n)
        b_refill(l, n_up + n)
        merge(n - 1)
        for i in range(2):
            h_copy(i).wait_send()
        merge(n)
        return carry

    lax.fori_loop(0, n_layers, layer, 0)
    out_copy = pltpu.make_async_copy(xs, x_out, csem.at[0])
    out_copy.start()
    out_copy.wait()


def hand_over(*refs):
    ins, outs, bufs, sem = refs[:3], refs[3:6], refs[6:9], refs[9]
    first = [pltpu.make_async_copy(ins[i], bufs[i], sem.at[i]) for i in range(3)]
    second = [pltpu.make_async_copy(bufs[i], outs[i], sem.at[i]) for i in range(3)]
    for copy in first:
        copy.start()
    for i in range(3):
        first[i].wait()
        second[i].start()
    for copy in second:
        copy.wait()


def solution(mesh):
    n_cp = mesh.shape["cp"]
    row_spec = P(("req", "cp"), None)
    tok_spec = P(("req", "cp"))
    rep_spec = P()
    cache_spec = P(None, "req", "cp")

    def local_step(hidden, positions, segments, gain_1, gain_2, w_q, w_k, w_v, w_o, w_1, w_3, w_2):
        n_layers, d_model, n_heads, head_dim = w_q.shape
        n_kv = w_k.shape[2]
        n_tok = hidden.shape[0]
        kvw = n_kv * head_dim
        q_group = n_heads // n_kv
        d_ff = w_1.shape[2]
        rows_a, cols_b, k_b, nb = kvw, d_model // 4, d_ff // 4, NB
        inv_freq = ROPE_THETA ** (-2.0 * jnp.arange(head_dim // 2, dtype=F32) / head_dim)
        angle = inv_freq[:, None] * positions.astype(F32)[None, :]
        cos_t, sin_t = jnp.cos(angle), jnp.sin(angle)

        def turned(w):
            return jnp.transpose(w, (0, 2, 3, 1)).reshape(n_layers, -1, d_model)

        cfg = dict(layers=n_layers, n_cp=n_cp, nb=nb)
        vmem = pl.BlockSpec(memory_space=pltpu.VMEM)
        hbm = pl.BlockSpec(memory_space=pl.ANY)
        n_all = n_cp * n_tok
        cache = jax.ShapeDtypeStruct((n_layers, kvw // n_cp, n_all), BF16)
        x, k_c, v_c = pl.pallas_call(
            functools.partial(kernel, cfg),
            out_shape=(jax.ShapeDtypeStruct(hidden.shape, BF16), cache, cache),
            in_specs=[hbm] + [vmem] * 5 + [hbm] * 7,
            out_specs=(hbm, hbm, hbm),
            scratch_shapes=[
                pltpu.VMEM((NA, rows_a, d_model), BF16),
                pltpu.VMEM((nb, k_b, cols_b), BF16),
                pltpu.VMEM((n_cp, 2 * kvw, n_tok), BF16),
                pltpu.VMEM((2 * kvw, 2 * n_tok), BF16),
                pltpu.VMEM((n_kv // 2, 2 * n_tok, 2 * head_dim), BF16),
                pltpu.VMEM((n_kv, 2 * head_dim, q_group * n_tok), BF16),
                pltpu.VMEM((n_kv, head_dim, q_group * n_tok), F32),
                pltpu.VMEM((n_kv, 8, q_group * n_tok), F32),
                pltpu.VMEM((n_kv, 8, q_group * n_tok), F32),
                pltpu.VMEM((2, 2 * n_tok, n_tok), F32),
                pltpu.VMEM((2, kvw // n_cp, n_all), BF16),
                pltpu.VMEM((n_tok, n_heads * head_dim), BF16),
                pltpu.VMEM((n_tok, d_model), BF16),
                pltpu.VMEM((2, n_tok, d_model), BF16),
                pltpu.VMEM((2 * n_tok, d_ff // 2), BF16),
                pltpu.VMEM((n_tok, d_model), F32),
                pltpu.VMEM((d_model // cols_b, n_tok, cols_b), F32),
                pltpu.VMEM((d_model // cols_b, n_tok, cols_b), F32),
                pltpu.VMEM((2, n_layers, 8, d_model), F32),
                pltpu.SemaphoreType.DMA((NA,)),
                pltpu.SemaphoreType.DMA((nb,)),
                pltpu.SemaphoreType.DMA((3, n_cp, 2)),
                pltpu.SemaphoreType.DMA((n_cp, 2)),
                pltpu.SemaphoreType.DMA((2, 2)),
                pltpu.SemaphoreType.DMA((2, 2)),
                pltpu.SemaphoreType.DMA((2,)),
                pltpu.SemaphoreType.DMA((2,)),
                pltpu.SemaphoreType.DMA((d_model // cols_b,)),
                pltpu.SemaphoreType.DMA((d_model // cols_b,)),
                pltpu.SemaphoreType.REGULAR((3,)),
                pltpu.SemaphoreType.DMA((2,)),
            ],
            compiler_params=pltpu.CompilerParams(
                collective_id=0, has_side_effects=True, vmem_limit_bytes=67043328),
            name="prefill",
        )(
            hidden, positions[None, :], cos_t, sin_t, gain_1, gain_2,
            turned(w_q), turned(w_k), turned(w_v), w_o.reshape(n_layers, -1, d_model), w_1, w_3, w_2,
        )
        results = (x, k_c, v_c)
        x, k_c, v_c = pl.pallas_call(
            hand_over,
            out_shape=tuple(jax.ShapeDtypeStruct(r.shape, r.dtype) for r in results),
            in_specs=[hbm] * 3,
            out_specs=(hbm,) * 3,
            scratch_shapes=[pltpu.VMEM(r.shape, r.dtype) for r in results] + [pltpu.SemaphoreType.DMA((3,))],
            name="hand_over",
        )(*results)
        return x, jnp.transpose(k_c, (0, 2, 1)), jnp.transpose(v_c, (0, 2, 1))

    return jax.shard_map(
        local_step,
        mesh=mesh,
        in_specs=(row_spec, tok_spec, tok_spec) + (rep_spec,) * 9,
        out_specs=(row_spec, cache_spec, cache_spec),
        check_vma=False,
    )
```
